128 devices in a mesh: zero: 32 (over y, x, core), width: 4 (over z).
Axes of the slice: x: 4, y: 4, z: 4, core: 2. Of those that a mesh axis runs over, the one named last changes fastest.
Arguments:
- train_query: bfloat16 [3584, 4096], P('zero', 'width'), may hold values from -0.09375 to 0.09375
- low_query: bfloat16 [3584, 32], P('zero'), may hold values from -0.09375 to 0.09375
- high_query: bfloat16 [32, 4096], P(None, 'width'), may hold values from -1 to 1
- train_key: bfloat16 [3584, 2048], P('zero', 'width'), may hold values from -0.09375 to 0.09375
- low_key: bfloat16 [3584, 32], P('zero'), may hold values from -0.09375 to 0.09375
- high_key: bfloat16 [32, 2048], P(None, 'width'), may hold values from -1 to 1
- train_value: bfloat16 [3584, 2048], P('zero', 'width'), may hold values from -0.09375 to 0.09375
- low_value: bfloat16 [3584, 32], P('zero'), may hold values from -0.09375 to 0.09375
- high_value: bfloat16 [32, 2048], P(None, 'width'), may hold values from -1 to 1
- train_mixed: bfloat16 [4096, 3584], P('width', 'zero'), may hold values from -0.09375 to 0.09375
- low_mixed: bfloat16 [4096, 32], P('width'), may hold values from -0.09375 to 0.09375
- high_mixed: bfloat16 [32, 3584], P(None, 'zero'), may hold values from -1 to 1
- norm_train: float32 [3584], P(('zero', 'width')), may hold values from 0.25 to 1.75
- norm_step: float32 [3584], P(('zero', 'width')), may hold values from -0.3 to 0.3
Outputs:
- ready_query: bfloat16 [4096, 3584], P('width')
- ready_key: bfloat16 [2048, 3584], P('width')
- ready_value: bfloat16 [2048, 3584], P('width')
- ready_mixed: bfloat16 [3584, 4096], P(None, 'width')
- serve_norm: bfloat16 [3584], replicated
The draws below stay inside these ranges and needn't reach their ends.
All inputs are finite; a program needn't handle non-finite values.
Results may differ from the reference program's by a relative error of at most 0.001.
Values may be sent and summed in bfloat16 or wider, within the bound.
No kernel may reach another device: no remote copies, remote signals or barrier semaphores. Data moves between devices by JAX's collectives and lax.ppermute only.
A program may use at most 128 MiB of HBM per device.

```python
import jax
import jax.numpy as jnp

D_MODEL = 3584
Q_DIM = 4096
KV_DIM = 2048
RANK = 32


def level_of(rng, extent, cuts, least, high):
    def one(dim, blocks):
        draws = jax.random.uniform(jax.random.fold_in(jax.random.fold_in(rng, 6), dim), (blocks,), jnp.float32, least / len(cuts), high / len(cuts))
        return jnp.repeat(jnp.exp(draws), extent[dim] // blocks).reshape((-1,) + (1,) * (len(extent) - dim - 1))

    gain = one(*cuts[0])
    for cut in cuts[1:]:
        gain = gain * one(*cut)
    return gain


def normal_values(own_key, extent, spread, most, cuts=(), held_as=jnp.bfloat16):
    drawn = jax.random.normal(own_key, extent, jnp.float32) * spread
    if len(cuts) > 0:
        drawn = level_of(own_key, extent, cuts, -0.22, 0.18) * drawn
    return jnp.clip(drawn, min=-most, max=most).astype(held_as)


def setup_inputs(seed: int = 0) -> dict:
    seeds = jax.random.split(jax.random.key(seed), 15)
    return {
        "train_query": normal_values(seeds[0], (D_MODEL, Q_DIM), D_MODEL ** -0.5, 0.09375, ((0, 32), (1, 4))),
        "low_query": normal_values(seeds[1], (D_MODEL, RANK), D_MODEL ** -0.5, 0.09375, ((0, 32),)),
        "high_query": normal_values(seeds[2], (RANK, Q_DIM), RANK ** -0.5, 1.0, ((1, 4),)),
        "train_key": normal_values(seeds[3], (D_MODEL, KV_DIM), D_MODEL ** -0.5, 0.09375, ((0, 32), (1, 4))),
        "low_key": normal_values(seeds[4], (D_MODEL, RANK), D_MODEL ** -0.5, 0.09375, ((0, 32),)),
        "high_key": normal_values(seeds[5], (RANK, KV_DIM), RANK ** -0.5, 1.0, ((1, 4),)),
        "train_value": normal_values(seeds[6], (D_MODEL, KV_DIM), D_MODEL ** -0.5, 0.09375, ((0, 32), (1, 4))),
        "low_value": normal_values(seeds[7], (D_MODEL, RANK), D_MODEL ** -0.5, 0.09375, ((0, 32),)),
        "high_value": normal_values(seeds[8], (RANK, KV_DIM), RANK ** -0.5, 1.0, ((1, 4),)),
        "train_mixed": normal_values(seeds[9], (Q_DIM, D_MODEL), Q_DIM ** -0.5, 0.09375, ((0, 4), (1, 32))),
        "low_mixed": normal_values(seeds[10], (Q_DIM, RANK), Q_DIM ** -0.5, 0.09375, ((0, 4),)),
        "high_mixed": normal_values(seeds[11], (RANK, D_MODEL), RANK ** -0.5, 1.0, ((1, 32),)),
        "norm_train": jnp.clip(1.0 + 0.15 * jax.random.normal(seeds[12], (D_MODEL,), jnp.float32), 0.25, 1.75),
        "norm_step": jnp.clip(jax.random.uniform(seeds[13], (D_MODEL,), jnp.float32, -0.3, 0.3) * level_of(seeds[13], (D_MODEL,), ((0, 128),), -0.4, 0.0), -0.3, 0.3),
    }


mix_rate = 0.5


def reference(train_query, low_query, high_query, train_key, low_key, high_key, train_value, low_value, high_value, train_mixed, low_mixed, high_mixed, norm_train, norm_step):
    latest_query = train_query.astype(jnp.float32) + mix_rate * jnp.dot(low_query, high_query, preferred_element_type=jnp.float32)
    latest_key = train_key.astype(jnp.float32) + mix_rate * jnp.dot(low_key, high_key, preferred_element_type=jnp.float32)
    latest_value = train_value.astype(jnp.float32) + mix_rate * jnp.dot(low_value, high_value, preferred_element_type=jnp.float32)
    latest_mixed = train_mixed.astype(jnp.float32) + mix_rate * jnp.dot(low_mixed, high_mixed, preferred_element_type=jnp.float32)
    ready_query = latest_query.T.astype(jnp.bfloat16)
    ready_key = latest_key.T.astype(jnp.bfloat16)
    ready_value = latest_value.T.astype(jnp.bfloat16)
    ready_mixed = latest_mixed.T.astype(jnp.bfloat16)
    serve_norm = (norm_train + norm_step).astype(jnp.bfloat16)
    return ready_query, ready_key, ready_value, ready_mixed, serve_norm
```

```python
import jax
import jax.numpy as jnp
from jax import lax
from jax.experimental import pallas as pl
from jax.experimental.pallas import tpu as pltpu
from jax.sharding import Mesh
from jax.sharding import PartitionSpec as P

ZERO = ("zero_0", "zero_1", "zero_2")
ZERO_WIDTH = ("zero_0", "zero_1", "zero_2", "width")


mix_rate = 0.5

ROWS = 112
HALF = 1536
CHUNK = 384
CHUNKS = 4
GROUP = 8 * ROWS
STRIP = 2 * ROWS
NORM = 28

ROUTE0 = (("query", 0, 1024), ("key", 0, 512))
ROUTE1 = (("value", 0, 512), ("mixed", 0, 1024))


def parts_of(route, chunk):
    low, high, at, found = chunk * CHUNK, (chunk + 1) * CHUNK, 0, []
    for name, _, width in route:
        first, last = max(low, at), min(high, at + width)
        if first < last:
            found.append((name, first - at, first - low, last - first))
        at += width
    return found


def pairs(move):
    return [
        ((y * 4 + x) * 2 + c, ((v % 4) * 4 + u % 4) * 2 + d)
        for y in range(4)
        for x in range(4)
        for c in range(2)
        for v, u, d in (move(y, x, c),)
    ]


def first_axis(step):
    return pairs(lambda y, x, c: (y, x + step, c) if c == 0 else (y + step, x, c))


def first_axis_across(step):
    return pairs(lambda y, x, c: (y, x + step, 0) if c == 1 else (y + step, x, 1))


def second_axis(step):
    return pairs(lambda y, x, c: (y + step, x, c) if c == 0 else (y, x + step, c))


PARTNER = pairs(lambda y, x, c: (y, x, 1 - c))


def send(array, to):
    return lax.ppermute(array, ZERO, to)


def place():
    return tuple(lax.axis_index(a) for a in ZERO)


def vmem(n):
    return [pl.BlockSpec(memory_space=pltpu.VMEM)] * n


def anywhere(n):
    return [pl.BlockSpec(memory_space=pl.ANY)] * n


def merge_kernel(
    tq, lq, hq, tk, lk, hk, tv, lv, hv, tm, lm, hm, gain, step, keep, give, line
):
    _, _, c = place()

    def latest(train, low, high):
        product = lax.dot_general(
            low[...], high[...], (((0,), (0,)), ((), ())), preferred_element_type=jnp.float32
        )
        return (train[...].astype(jnp.float32) + mix_rate * product).astype(jnp.bfloat16)

    line[...] = jnp.zeros(line.shape, jnp.float32)
    line[0:1, 0:NORM] = gain[...] + step[...]
    rows = slice(0, ROWS)
    for to in (keep, give):
        to[ROWS : ROWS + 8, 0:128] = line[...].astype(jnp.bfloat16)

    def fill(first, second):
        first[rows, 0:1024] = latest(tq, lq, hq)
        first[rows, 1024:1536] = latest(tk, lk, hk)
        second[rows, 0:512] = latest(tv, lv, hv)
        second[rows, 512:1536] = latest(tm, lm, hm)

    @pl.when(c == 0)
    def _():
        fill(keep, give)

    @pl.when(c == 1)
    def _():
        fill(give, keep)


def merge(*args):
    piece = jax.ShapeDtypeStruct((ROWS + 8, HALF), jnp.bfloat16)
    return pl.pallas_call(
        merge_kernel,
        out_shape=(piece, piece),
        in_specs=vmem(len(args)),
        out_specs=tuple(vmem(2)),
        scratch_shapes=[pltpu.VMEM((8, 128), jnp.float32)],
        name="merge",
    )(*args)


OFFSETS = ((0, 0), (0, 1), (-1, 0), (1, 0), (-1, 1), (1, 1), (2, 0), (2, 1))


def stack_kernel(*refs):
    pieces, chunks, lines = refs[:8], refs[8:12], refs[12]
    y, x, c = place()
    a = jnp.where(c == 0, x, y)
    for piece, (step, other) in zip(pieces, OFFSETS):
        core = c if other == 0 else 1 - c
        at = ((a + step + 4) % 4) * 2 + core
        for j in range(CHUNKS):
            chunks[j][pl.ds(pl.multiple_of(at * ROWS, 16), ROWS), :] = piece[
                0:ROWS, j * CHUNK : (j + 1) * CHUNK
            ]
        lines[pl.ds(at, 1), :] = piece[ROWS : ROWS + 8, 0:128].astype(jnp.float32)[0:1]
    chunks[0][GROUP : GROUP + 8, 0:128] = lines[...].astype(jnp.bfloat16)


def stack(pieces):
    return pl.pallas_call(
        stack_kernel,
        out_shape=tuple(
            jax.ShapeDtypeStruct((GROUP + (8 if j == 0 else 0), CHUNK), jnp.bfloat16)
            for j in range(CHUNKS)
        ),
        in_specs=vmem(8),
        out_specs=tuple(vmem(CHUNKS)),
        scratch_shapes=[pltpu.VMEM((8, 128), jnp.float32)],
        name="stack",
    )(*pieces)


NAMES = ("query", "key", "mixed")
SHAPES = {"query": (1024, 3584), "key": (512, 3584), "mixed": (3584, 1024)}


def lay_kernel(work, n_in, *refs):
    units, refs = refs[: 2 * len(work)], refs[2 * len(work) + n_in :]
    outs, (turned, sems) = dict(zip(NAMES, refs[:3])), refs[3:]
    y, x, c = place()

    def lay(route0, route1):
        started = []

        def start(source, target):
            copy = pltpu.make_async_copy(source, target, sems.at[len(started)])
            copy.start()
            started.append(copy)

        for (step, chunk), unit in zip(work, route1):
            g = (x + step + 4) % 4
            for name, first, at, width in parts_of(ROUTE1, chunk):
                if name == "mixed":
                    for s in range(4):
                        row = pl.multiple_of(s * GROUP + g * STRIP, 16)
                        start(
                            unit.at[pl.ds(s * STRIP, STRIP), pl.ds(at, width)],
                            outs[name].at[pl.ds(row, STRIP), pl.ds(first, width)],
                        )
        for i, ((step, chunk), unit) in enumerate(zip(work, route0)):
            g = (y + step + 4) % 4
            turned[i] = unit[0:GROUP, :].T
            for name, first, at, width in parts_of(ROUTE0, chunk):
                column = pl.multiple_of(g * GROUP, 128)
                start(
                    turned.at[i, pl.ds(at, width), :],
                    outs[name].at[pl.ds(first, width), pl.ds(column, GROUP)],
                )
        for copy in started:
            copy.wait()

    half = len(work)

    @pl.when(c == 0)
    def _():
        lay(units[:half], units[half:])

    @pl.when(c == 1)
    def _():
        lay(units[half:], units[:half])


def lay(work, own, partner, before):
    n = len(work)
    n_in = 0 if before is None else 3
    shapes = tuple(jax.ShapeDtypeStruct(SHAPES[name], jnp.bfloat16) for name in NAMES)
    return pl.pallas_call(
        lambda *refs: lay_kernel(work, n_in, *refs),
        out_shape=shapes,
        in_specs=vmem(2 * n) + anywhere(n_in),
        out_specs=tuple(anywhere(3)),
        scratch_shapes=[
            pltpu.VMEM((n, CHUNK, GROUP), jnp.bfloat16),
            pltpu.SemaphoreType.DMA((6 * n,)),
        ],
        input_output_aliases={2 * n + i: i for i in range(n_in)},
        name="lay_" + "_".join(f"{s + 1}{j}" for s, j in work),
    )(*own, *partner, *(before or ()))


STEPS = (0, -1, 1, 2)


def value_kernel(*refs):
    units, out, whole, turned, sems = refs[:16], refs[16], refs[17], refs[18], refs[19]
    y, x, c = place()

    def gather(mine):
        for k, step in enumerate(STEPS):
            g = (x + step + 4) % 4
            for chunk in range(2):
                for name, first, at, width in parts_of(ROUTE1, chunk):
                    if name == "value":
                        for s in range(4):
                            row = pl.multiple_of(s * GROUP + g * STRIP, 16)
                            whole[pl.ds(row, STRIP), first : first + width] = mine[2 * k + chunk][
                                s * STRIP : (s + 1) * STRIP, at : at + width
                            ]

    @pl.when(c == 0)
    def _():
        gather(units[8:])

    @pl.when(c == 1)
    def _():
        gather(units[:8])

    copies = []
    for s in range(4):
        turned[s] = whole[s * GROUP : (s + 1) * GROUP, :].T
        copy = pltpu.make_async_copy(turned.at[s], out.at[:, pl.ds(s * GROUP, GROUP)], sems.at[s])
        copy.start()
        copies.append(copy)
    for copy in copies:
        copy.wait()


def value_of(own, partner):
    return pl.pallas_call(
        value_kernel,
        out_shape=jax.ShapeDtypeStruct((512, 3584), jnp.bfloat16),
        in_specs=vmem(16),
        out_specs=pl.BlockSpec(memory_space=pl.ANY),
        scratch_shapes=[
            pltpu.VMEM((3584, 512), jnp.bfloat16),
            pltpu.VMEM((4, 512, GROUP), jnp.bfloat16),
            pltpu.SemaphoreType.DMA((4,)),
        ],
        name="value",
    )(*own, *partner)


def lines_kernel(*refs):
    units, out, rows = refs[:4], refs[4], refs[5]
    y, x, c = place()
    b = jnp.where(c == 0, y, x)
    for unit, step in zip(units, STEPS):
        g = (b + step + 4) % 4
        found = unit[GROUP : GROUP + 8, 0:128].astype(jnp.float32)
        for p in range(8):
            at = jnp.where(c == 0, g * 8 + p, (p // 2) * 8 + g * 2 + p % 2)
            rows[pl.ds(at, 1), :] = found[p : p + 1]
    out[...] = rows[...].astype(jnp.bfloat16)


def lines_of(units):
    return pl.pallas_call(
        lines_kernel,
        out_shape=jax.ShapeDtypeStruct((32, 128), jnp.bfloat16),
        in_specs=vmem(4),
        out_specs=pl.BlockSpec(memory_space=pltpu.VMEM),
        scratch_shapes=[pltpu.VMEM((32, 128), jnp.float32)],
        name="lines",
    )(*units)


def body(
    train_query,
    low_query,
    high_query,
    train_key,
    low_key,
    high_key,
    train_value,
    low_value,
    high_value,
    train_mixed,
    low_mixed,
    high_mixed,
    norm_train,
    norm_step,
):
    keep, give = merge(
        train_query,
        low_query.T,
        high_query,
        train_key,
        low_key.T,
        high_key,
        train_value,
        low_value.T,
        high_value,
        train_mixed.T,
        high_mixed,
        low_mixed.T,
        norm_train.reshape(1, NORM),
        norm_step.reshape(1, NORM),
    )
    beside = send(give, PARTNER)
    keep_up, give_down = send(keep, first_axis(1)), send(give, first_axis_across(-1))
    keep_down, give_up = send(keep, first_axis(-1)), send(give, first_axis_across(1))
    far_keep, far_give = send(keep_up, first_axis(1)), send(give_down, first_axis(-1))
    group = stack(
        (keep, beside, keep_up, keep_down, give_up, give_down, far_keep, far_give)
    )
    up = [send(g, second_axis(1)) for g in group]
    down = [send(g, second_axis(-1)) for g in group]
    far = [
        send(up[j], second_axis(1)) if j % 2 == 0 else send(down[j], second_axis(-1))
        for j in range(CHUNKS)
    ]
    mine = {0: group, -1: up, 1: down, 2: far}
    theirs = {s: [send(u, PARTNER) for u in mine[s]] for s in STEPS}

    outs = None
    for work in (
        ((0, 0), (0, 1), (0, 2), (0, 3)),
        ((-1, 0), (1, 0), (-1, 1), (1, 1)),
        ((-1, 2), (1, 2), (-1, 3), (1, 3)),
        ((2, 0), (2, 1)),
        ((2, 2), (2, 3)),
    ):
        outs = lay(work, [mine[s][j] for s, j in work], [theirs[s][j] for s, j in work], outs)
    ready_query, ready_key, ready_mixed = outs
    ready_value = value_of(
        [mine[s][j] for s in STEPS for j in range(2)],
        [theirs[s][j] for s in STEPS for j in range(2)],
    )

    lines = lines_of([mine[s][0] for s in STEPS])
    ring = [[(i, (i + k) % 4) for i in range(4)] for k in range(4)]
    around = [lines] + [lax.ppermute(lines, "width", ring[4 - k]) for k in range(1, 4)]
    twice = jnp.stack(around + around)[:, :, :NORM]
    z = lax.axis_index("width")
    ordered = lax.dynamic_slice(twice, ((4 - z) % 4, 0, 0), (4, 32, NORM))
    serve_norm = ordered.transpose(1, 0, 2).reshape(-1)
    return (ready_query, ready_key, ready_value, ready_mixed, serve_norm)


def solution(mesh):
    torus = Mesh(
        mesh.devices.reshape(4, 4, 2, mesh.shape["width"]), ("zero_0", "zero_1", "zero_2", "width")
    )
    return jax.shard_map(
        body,
        mesh=torus,
        in_specs=(
            P(ZERO, "width"),
            P(ZERO, None),
            P(None, "width"),
            P(ZERO, "width"),
            P(ZERO, None),
            P(None, "width"),
            P(ZERO, "width"),
            P(ZERO, None),
            P(None, "width"),
            P("width", ZERO),
            P("width", None),
            P(None, ZERO),
            P(ZERO_WIDTH),
            P(ZERO_WIDTH),
        ),
        out_specs=(P("width", None), P("width", None), P("width", None), P(None, "width"), P()),
        check_vma=False,
    )
```

```python
import jax
import jax.numpy as jnp
from jax import lax
from jax.experimental import pallas as pl
from jax.experimental.pallas import tpu as pltpu
from jax.sharding import Mesh
from jax.sharding import PartitionSpec as P

ZERO = ("zero_0", "zero_1", "zero_2")
ZERO_WIDTH = ("zero_0", "zero_1", "zero_2", "width")


mix_rate = 0.5

ROWS = 112
HALF = 1536
CHUNK = 384
CHUNKS = 4
GROUP = 8 * ROWS
STRIP = 2 * ROWS
NORM = 28

ROUTE0 = (("query", 0, 1024), ("key", 0, 512))
ROUTE1 = (("value", 0, 512), ("mixed", 0, 1024))


def parts_of(route, chunk):
    low, high, at, found = chunk * CHUNK, (chunk + 1) * CHUNK, 0, []
    for name, _, width in route:
        first, last = max(low, at), min(high, at + width)
        if first < last:
            found.append((name, first - at, first - low, last - first))
        at += width
    return found


def pairs(move):
    return [
        ((y * 4 + x) * 2 + c, ((v % 4) * 4 + u % 4) * 2 + d)
        for y in range(4)
        for x in range(4)
        for c in range(2)
        for v, u, d in (move(y, x, c),)
    ]


def first_axis(step):
    return pairs(lambda y, x, c: (y, x + step, c) if c == 0 else (y + step, x, c))


def first_axis_across(step):
    return pairs(lambda y, x, c: (y, x + step, 0) if c == 1 else (y + step, x, 1))


def second_axis(step):
    return pairs(lambda y, x, c: (y + step, x, c) if c == 0 else (y, x + step, c))


PARTNER = pairs(lambda y, x, c: (y, x, 1 - c))


def send(array, to):
    return lax.ppermute(array, ZERO, to)


def place():
    return tuple(lax.axis_index(a) for a in ZERO)


def held(arrays):
    return [pltpu.with_memory_space_constraint(a, pltpu.VMEM) for a in arrays]


def vmem(n):
    return [pl.BlockSpec(memory_space=pltpu.VMEM)] * n


def anywhere(n):
    return [pl.BlockSpec(memory_space=pl.ANY)] * n


MERGED = (
    (ROWS, 1024), (32, ROWS), (32, 1024),
    (ROWS, 512), (32, ROWS), (32, 512),
    (ROWS, 512), (32, ROWS), (32, 512),
    (ROWS, 1024), (32, ROWS), (32, 1024),
    (1, NORM), (1, NORM),
)


def merge_kernel(*refs):
    ins, (keep, give), here, line, sems = refs[:14], refs[14:16], refs[16:30], refs[30], refs[31]
    _, _, c = place()
    copies = [pltpu.make_async_copy(a, b, sems.at[i]) for i, (a, b) in enumerate(zip(ins, here))]
    for copy in copies:
        copy.start()
    line[...] = jnp.zeros(line.shape, jnp.float32)
    for copy in copies:
        copy.wait()
    tq, lq, hq, tk, lk, hk, tv, lv, hv, tm, lm, hm, gain, step = here

    def latest(train, low, high):
        product = lax.dot_general(
            low[...], high[...], (((0,), (0,)), ((), ())), preferred_element_type=jnp.float32
        )
        return (train[...].astype(jnp.float32) + mix_rate * product).astype(jnp.bfloat16)

    line[0:1, 0:NORM] = gain[...] + step[...]
    rows = slice(0, ROWS)
    for to in (keep, give):
        to[ROWS : ROWS + 8, 0:128] = line[...].astype(jnp.bfloat16)

    def fill(first, second):
        first[rows, 0:1024] = latest(tq, lq, hq)
        first[rows, 1024:1536] = latest(tk, lk, hk)
        second[rows, 0:512] = latest(tv, lv, hv)
        second[rows, 512:1536] = latest(tm, lm, hm)

    @pl.when(c == 0)
    def _():
        fill(keep, give)

    @pl.when(c == 1)
    def _():
        fill(give, keep)


def merge(*args):
    piece = pltpu.VMEM((ROWS + 8, HALF), jnp.bfloat16)
    return pl.pallas_call(
        merge_kernel,
        out_shape=(piece, piece),
        in_specs=anywhere(len(args)),
        out_specs=tuple(vmem(2)),
        scratch_shapes=[pltpu.VMEM(shape, a.dtype) for shape, a in zip(MERGED, args)]
        + [pltpu.VMEM((8, 128), jnp.float32), pltpu.SemaphoreType.DMA((14,))],
        compiler_params=pltpu.CompilerParams(vmem_limit_bytes=8 * 2**20),
        name="merge",
    )(*[pltpu.with_memory_space_constraint(a, pltpu.HBM) for a in args])


OFFSETS = ((0, 0), (0, 1), (-1, 0), (1, 0), (-1, 1), (1, 1), (2, 0), (2, 1))


def stack_kernel(*refs):
    pieces, chunks, lines = refs[:8], refs[8:12], refs[12]
    y, x, c = place()
    a = jnp.where(c == 0, x, y)
    for piece, (step, other) in zip(pieces, OFFSETS):
        core = c if other == 0 else 1 - c
        at = ((a + step + 4) % 4) * 2 + core
        for j in range(CHUNKS):
            chunks[j][pl.ds(pl.multiple_of(at * ROWS, 16), ROWS), :] = piece[
                0:ROWS, j * CHUNK : (j + 1) * CHUNK
            ]
        lines[pl.ds(at, 1), :] = piece[ROWS : ROWS + 8, 0:128].astype(jnp.float32)[0:1]
    chunks[0][GROUP : GROUP + 8, 0:128] = lines[...].astype(jnp.bfloat16)


def stack(pieces):
    return pl.pallas_call(
        stack_kernel,
        out_shape=tuple(
            pltpu.VMEM((GROUP + (8 if j == 0 else 0), CHUNK), jnp.bfloat16)
            for j in range(CHUNKS)
        ),
        in_specs=vmem(8),
        out_specs=tuple(vmem(CHUNKS)),
        scratch_shapes=[pltpu.VMEM((8, 128), jnp.float32)],
        compiler_params=pltpu.CompilerParams(vmem_limit_bytes=4 * 2**20),
        name="stack",
    )(*held(pieces))


NAMES = ("query", "key", "mixed")
SHAPES = {"query": (1024, 3584), "key": (512, 3584), "mixed": (3584, 1024)}


def lay_kernel(work, n_in, *refs):
    units, refs = refs[: 2 * len(work)], refs[2 * len(work) + n_in :]
    outs, (turned, sems) = dict(zip(NAMES, refs[:3])), refs[3:]
    y, x, c = place()

    def lay(route0, route1):
        started = []

        def start(source, target):
            copy = pltpu.make_async_copy(source, target, sems.at[len(started)])
            copy.start()
            started.append(copy)

        for (step, chunk), unit in zip(work, route1):
            g = (x + step + 4) % 4
            for name, first, at, width in parts_of(ROUTE1, chunk):
                if name == "mixed":
                    for s in range(4):
                        row = pl.multiple_of(s * GROUP + g * STRIP, 16)
                        start(
                            unit.at[pl.ds(s * STRIP, STRIP), pl.ds(at, width)],
                            outs[name].at[pl.ds(row, STRIP), pl.ds(first, width)],
                        )
        for i, ((step, chunk), unit) in enumerate(zip(work, route0)):
            g = (y + step + 4) % 4
            turned[i] = unit[0:GROUP, :].T
            for name, first, at, width in parts_of(ROUTE0, chunk):
                column = pl.multiple_of(g * GROUP, 128)
                start(
                    turned.at[i, pl.ds(at, width), :],
                    outs[name].at[pl.ds(first, width), pl.ds(column, GROUP)],
                )
        for copy in started:
            copy.wait()

    half = len(work)

    @pl.when(c == 0)
    def _():
        lay(units[:half], units[half:])

    @pl.when(c == 1)
    def _():
        lay(units[half:], units[:half])


LAID = (
    ((0, 0), (0, 1), (0, 2), (0, 3)),
    ((-1, 0), (1, 0), (-1, 1), (1, 1)),
    ((2, 0), (2, 1)),
    ((-1, 2), (1, 2), (-1, 3), (1, 3)),
    ((2, 2), (2, 3)),
)


def lay(work, own, partner, before):
    n = len(work)
    n_in = 0 if before is None else 3
    shapes = tuple(jax.ShapeDtypeStruct(SHAPES[name], jnp.bfloat16) for name in NAMES)
    return pl.pallas_call(
        lambda *refs: lay_kernel(work, n_in, *refs),
        out_shape=shapes,
        in_specs=vmem(2 * n) + anywhere(n_in),
        out_specs=tuple(anywhere(3)),
        scratch_shapes=[
            pltpu.VMEM((n, CHUNK, GROUP), jnp.bfloat16),
            pltpu.SemaphoreType.DMA((6 * n,)),
        ],
        input_output_aliases={2 * n + i: i for i in range(n_in)},
        compiler_params=pltpu.CompilerParams(vmem_limit_bytes=12 * 2**20),
    )(*held(own), *held(partner), *(before or ()))


STEPS = (0, -1, 1, 2)


def value_kernel(*refs):
    units, out, whole, turned, sems = refs[:16], refs[16], refs[17], refs[18], refs[19]
    _, x, c = place()

    def gather(mine):
        for k, step in enumerate(STEPS):
            g = (x + step + 4) % 4
            for chunk in range(2):
                for name, first, at, width in parts_of(ROUTE1, chunk):
                    if name == "value":
                        for s in range(4):
                            row = pl.multiple_of(s * GROUP + g * STRIP, 16)
                            whole[pl.ds(row, STRIP), first : first + width] = mine[2 * k + chunk][
                                s * STRIP : (s + 1) * STRIP, at : at + width
                            ]

    @pl.when(c == 0)
    def _():
        gather(units[8:])

    @pl.when(c == 1)
    def _():
        gather(units[:8])

    copies = []
    for s in range(4):
        turned[s] = whole[s * GROUP : (s + 1) * GROUP, :].T
        copy = pltpu.make_async_copy(turned.at[s], out.at[:, pl.ds(s * GROUP, GROUP)], sems.at[s])
        copy.start()
        copies.append(copy)
    for copy in copies:
        copy.wait()


def value_of(own, partner):
    return pl.pallas_call(
        value_kernel,
        out_shape=jax.ShapeDtypeStruct((512, 3584), jnp.bfloat16),
        in_specs=vmem(16),
        out_specs=pl.BlockSpec(memory_space=pl.ANY),
        scratch_shapes=[
            pltpu.VMEM((3584, 512), jnp.bfloat16),
            pltpu.VMEM((4, 512, GROUP), jnp.bfloat16),
            pltpu.SemaphoreType.DMA((4,)),
        ],
        compiler_params=pltpu.CompilerParams(vmem_limit_bytes=16 * 2**20),
        name="value",
    )(*held(own), *held(partner))


def lines_kernel(*refs):
    units, out, rows = refs[:4], refs[4], refs[5]
    y, x, c = place()
    b = jnp.where(c == 0, y, x)
    for unit, step in zip(units, STEPS):
        g = (b + step + 4) % 4
        found = unit[GROUP : GROUP + 8, 0:128].astype(jnp.float32)
        for p in range(8):
            at = jnp.where(c == 0, g * 8 + p, (p // 2) * 8 + g * 2 + p % 2)
            rows[pl.ds(at, 1), :] = found[p : p + 1]
    out[...] = rows[...].astype(jnp.bfloat16)


def lines_of(units):
    return pl.pallas_call(
        lines_kernel,
        out_shape=jax.ShapeDtypeStruct((32, 128), jnp.bfloat16),
        in_specs=vmem(4),
        out_specs=pl.BlockSpec(memory_space=pltpu.VMEM),
        scratch_shapes=[pltpu.VMEM((32, 128), jnp.float32)],
        compiler_params=pltpu.CompilerParams(vmem_limit_bytes=4 * 2**20),
        name="lines",
    )(*held(units))


def norm_kernel(here, last, beyond, following, out, rows):
    z = lax.axis_index("width")
    at = lax.broadcasted_iota(jnp.int32, (128, 32), 0)
    piece = lax.broadcasted_iota(jnp.int32, (128, 32), 1)
    found = jnp.zeros((128, 128), jnp.float32)
    for step, ref in enumerate((here, last, beyond, following)):
        pick = (at == piece * 4 + (z - step + 4) % 4).astype(jnp.float32).astype(jnp.bfloat16)
        found += jnp.dot(pick, ref[...], preferred_element_type=jnp.float32)
    start = lax.broadcasted_iota(jnp.int32, (128, 128), 0) * NORM
    lane = lax.broadcasted_iota(jnp.int32, (128, 128), 1)
    column = (lane - start) & 127
    row = jnp.where(column < NORM, (start + column) >> 7, 128)
    turned = jnp.zeros((128, 128), jnp.float32)
    for k in range(NORM):
        turned = jnp.where(column == k, found[:, k : k + 1], turned)
    rows[...] = jnp.zeros(rows.shape, jnp.float32)
    for r in range(28):
        rows[r : r + 1, :] = jnp.sum(jnp.where(row == r, turned, 0.0), axis=0, keepdims=True)
    out[...] = rows[0:28, :].astype(jnp.bfloat16)


def norm_of(lines):
    return pl.pallas_call(
        norm_kernel,
        out_shape=jax.ShapeDtypeStruct((28, 128), jnp.bfloat16),
        in_specs=vmem(4),
        out_specs=pl.BlockSpec(memory_space=pltpu.VMEM),
        scratch_shapes=[pltpu.VMEM((32, 128), jnp.float32)],
        compiler_params=pltpu.CompilerParams(vmem_limit_bytes=4 * 2**20),
        name="norm",
    )(*held(lines))


def body(
    train_query,
    low_query,
    high_query,
    train_key,
    low_key,
    high_key,
    train_value,
    low_value,
    high_value,
    train_mixed,
    low_mixed,
    high_mixed,
    norm_train,
    norm_step,
):
    keep, give = merge(
        train_query,
        low_query.T,
        high_query,
        train_key,
        low_key.T,
        high_key,
        train_value,
        low_value.T,
        high_value,
        train_mixed.T,
        high_mixed,
        low_mixed.T,
        norm_train.reshape(1, NORM),
        norm_step.reshape(1, NORM),
    )
    beside = send(give, PARTNER)
    keep_up = send(keep, first_axis(1))
    give_down = send(give, first_axis_across(-1))
    keep_down = send(keep, first_axis(-1))
    give_up = send(give, first_axis_across(1))
    far_keep = send(keep_up, first_axis(1))
    far_give = send(give_down, first_axis(-1))
    group = stack((keep, beside, keep_up, keep_down, give_up, give_down, far_keep, far_give))
    mine = {
        0: group,
        -1: [send(g, second_axis(1)) for g in group],
        1: [send(g, second_axis(-1)) for g in group],
    }
    mine[2] = [
        send(mine[-1 if j % 2 == 0 else 1][j], second_axis(1 if j % 2 == 0 else -1))
        for j in range(CHUNKS)
    ]
    theirs = {s: [send(u, PARTNER) for u in mine[s]] for s in STEPS}

    outs = None
    for work in LAID:
        own, partner = [mine[s][j] for s, j in work], [theirs[s][j] for s, j in work]
        outs = lay(work, own, partner, outs)
    ready_query, ready_key, ready_mixed = outs
    ready_value = value_of(
        [mine[s][j] for s in STEPS for j in range(2)],
        [theirs[s][j] for s in STEPS for j in range(2)],
    )

    lines = lines_of([mine[s][0] for s in STEPS])
    around = [lines]
    for k in range(1, 4):
        to = [(i, (i + k) % 4) for i in range(4)]
        around.append(lax.ppermute(lines, "width", to))
    serve_norm = norm_of(around).reshape(-1)
    return (ready_query, ready_key, ready_value, ready_mixed, serve_norm)


def solution(mesh):
    torus = Mesh(
        mesh.devices.reshape(4, 4, 2, mesh.shape["width"]), ("zero_0", "zero_1", "zero_2", "width")
    )
    return jax.shard_map(
        body,
        mesh=torus,
        in_specs=(
            P(ZERO, "width"),
            P(ZERO, None),
            P(None, "width"),
            P(ZERO, "width"),
            P(ZERO, None),
            P(None, "width"),
            P(ZERO, "width"),
            P(ZERO, None),
            P(None, "width"),
            P("width", ZERO),
            P("width", None),
            P(None, ZERO),
            P(ZERO_WIDTH),
            P(ZERO_WIDTH),
        ),
        out_specs=(P("width", None), P("width", None), P("width", None), P(None, "width"), P()),
        check_vma=False,
    )
```

```python
import jax
import jax.numpy as jnp
from jax import lax
from jax.experimental import pallas as pl
from jax.experimental.pallas import tpu as pltpu
from jax.sharding import Mesh
from jax.sharding import PartitionSpec as P

ZERO = ("zero_0", "zero_1", "zero_2")
ZERO_WIDTH = ("zero_0", "zero_1", "zero_2", "width")


mix_rate = 0.5

ROWS = 112
HALF = 1536
WIDTHS = (512, 768, 256)
FIRSTS = (0, 512, 1280)
CHUNKS = 3
GROUP = 8 * ROWS
STRIP = 2 * ROWS
REST = 3 * STRIP
NORM = 28

ROUTE0 = (
    (("query", 0, 0, 512),),
    (("query", 512, 0, 512), ("key", 0, 512, 256)),
    (("key", 256, 0, 256),),
)
ROUTE1 = ((("value", 0, 0, 512),), (("mixed", 0, 0, 768),), (("mixed", 768, 0, 256),))


def columns(j):
    return slice(FIRSTS[j], FIRSTS[j] + WIDTHS[j])


def pairs(move):
    return [
        ((y * 4 + x) * 2 + c, ((v % 4) * 4 + u % 4) * 2 + d)
        for y in range(4)
        for x in range(4)
        for c in range(2)
        for v, u, d in (move(y, x, c),)
    ]


def first_axis(step):
    return pairs(lambda y, x, c: (y, x + step, c) if c == 0 else (y + step, x, c))


def first_axis_across(step):
    return pairs(lambda y, x, c: (y, x + step, 0) if c == 1 else (y + step, x, 1))


def second_axis(step):
    return pairs(lambda y, x, c: (y + step, x, c) if c == 0 else (y, x + step, c))


PARTNER = pairs(lambda y, x, c: (y, x, 1 - c))


def send(array, to):
    return lax.ppermute(array, ZERO, to)


def place():
    return tuple(lax.axis_index(a) for a in ZERO)


def held(arrays):
    return [pltpu.with_memory_space_constraint(a, pltpu.VMEM) for a in arrays]


def vmem(n):
    return [pl.BlockSpec(memory_space=pltpu.VMEM)] * n


def anywhere(n):
    return [pl.BlockSpec(memory_space=pl.ANY)] * n


MERGED = (
    (ROWS, 1024), (32, ROWS), (32, 1024),
    (ROWS, 512), (32, ROWS), (32, 512),
    (ROWS, 512), (32, ROWS), (32, 512),
    (ROWS, 1024), (32, ROWS), (32, 1024),
    (1, NORM), (1, NORM),
)


def merge_kernel(*refs):
    ins, (keep, give, norm), here, (line, sems) = refs[:14], refs[14:17], refs[17:31], refs[31:]
    y, x, c = place()
    copies = [pltpu.make_async_copy(a, b, sems.at[i]) for i, (a, b) in enumerate(zip(ins, here))]
    for copy in copies:
        copy.start()
    line[...] = jnp.zeros(line.shape, jnp.float32)
    for copy in copies:
        copy.wait()
    tq, lq, hq, tk, lk, hk, tv, lv, hv, tm, lm, hm, gain, step = here

    def latest(train, low, high):
        product = lax.dot_general(
            low[...], high[...], (((0,), (0,)), ((), ())), preferred_element_type=jnp.float32
        )
        return (train[...].astype(jnp.float32) + mix_rate * product).astype(jnp.bfloat16)

    first = ((((y * 4 + x) * 2 + c) * 4) + lax.axis_index("width")) * NORM
    row, at = first // 128, first % 128
    lane = lax.broadcasted_iota(jnp.int32, (1, 128), 1)
    line[0:1, 0:NORM] = gain[...] + step[...]
    turned = pltpu.roll(line[0:1, :], at, 1)
    line[0:1, :] = jnp.zeros((1, 128), jnp.float32)
    line[pl.ds(row, 1), :] = jnp.where(lane >= at, turned, 0.0)
    line[pl.ds(row + 1, 1), :] = jnp.where(lane < at, turned, line[pl.ds(row + 1, 1), :])
    norm[...] = line[...].astype(jnp.bfloat16)

    rows = slice(0, ROWS)

    def fill(first, second):
        first[rows, 0:1024] = latest(tq, lq, hq)
        first[rows, 1024:1536] = latest(tk, lk, hk)
        second[rows, 0:512] = latest(tv, lv, hv)
        second[rows, 512:1536] = latest(tm, lm, hm)

    @pl.when(c == 0)
    def _():
        fill(keep, give)

    @pl.when(c == 1)
    def _():
        fill(give, keep)


def merge(*args):
    piece = pltpu.VMEM((ROWS, HALF), jnp.bfloat16)
    return pl.pallas_call(
        merge_kernel,
        out_shape=(piece, piece, pltpu.VMEM((32, 128), jnp.bfloat16)),
        in_specs=anywhere(len(args)),
        out_specs=tuple(vmem(3)),
        scratch_shapes=[pltpu.VMEM(shape, a.dtype) for shape, a in zip(MERGED, args)]
        + [pltpu.VMEM((32, 128), jnp.float32), pltpu.SemaphoreType.DMA((14,))],
        compiler_params=pltpu.CompilerParams(vmem_limit_bytes=8 * 2**20),
        name="merge",
    )(*[pltpu.with_memory_space_constraint(a, pltpu.HBM) for a in args])


def pair_kernel(keep, beside, out):
    _, _, c = place()
    for piece, core in ((keep, c), (beside, 1 - c)):
        out[pl.ds(pl.multiple_of(core * ROWS, 16), ROWS), :] = piece[...]


def pair_of(keep, beside):
    return pl.pallas_call(
        pair_kernel,
        out_shape=pltpu.VMEM((STRIP, HALF), jnp.bfloat16),
        in_specs=vmem(2),
        out_specs=pl.BlockSpec(memory_space=pltpu.VMEM),
        compiler_params=pltpu.CompilerParams(vmem_limit_bytes=2 * 2**20),
        name="pair",
    )(*held((keep, beside)))


OFFSETS = ((3, 0), (1, 0), (3, 1), (1, 1), (2, 0), (2, 1))


def stack_kernel(*refs):
    pieces, chunks = refs[:6], refs[6:]
    _, _, c = place()
    for piece, (step, other) in zip(pieces, OFFSETS):
        core = c if other == 0 else 1 - c
        at = pl.multiple_of(((step - 1) * 2 + core) * ROWS, 16)
        for j in range(CHUNKS):
            chunks[j][pl.ds(at, ROWS), :] = piece[:, columns(j)]


def stack(pieces):
    return pl.pallas_call(
        stack_kernel,
        out_shape=tuple(pltpu.VMEM((REST, width), jnp.bfloat16) for width in WIDTHS),
        in_specs=vmem(6),
        out_specs=tuple(vmem(CHUNKS)),
        compiler_params=pltpu.CompilerParams(vmem_limit_bytes=4 * 2**20),
        name="stack",
    )(*held(pieces))


NAMES = ("query", "key", "mixed")
SHAPES = {"query": (1024, 3584), "key": (512, 3584), "mixed": (3584, 1024)}


def lay_kernel(work, n_in, *refs):
    units, refs = refs[: 4 * len(work)], refs[4 * len(work) + n_in :]
    outs, scratch, sems = dict(zip(NAMES, refs[:3])), refs[3:-1], refs[-1]
    y, x, c = place()

    def lay(route0, route1):
        started = []

        def start(source, target):
            copy = pltpu.make_async_copy(source, target, sems.at[len(started)])
            copy.start()
            started.append(copy)

        for (step, j), (pair, rest) in zip(work, route1):
            for name, first, at, width in ROUTE1[j]:
                if name != "mixed":
                    continue
                g = (x + step + 4) % 4
                for k in range(4):
                    row = pl.multiple_of(((y + k) % 4) * GROUP + g * STRIP, 16)
                    source = (
                        pair.at[:, pl.ds(FIRSTS[j] + at, width)]
                        if k == 0
                        else rest.at[pl.ds((k - 1) * STRIP, STRIP), pl.ds(at, width)]
                    )
                    start(source, outs[name].at[pl.ds(row, STRIP), pl.ds(first, width)])
        for i, ((step, j), (pair, rest)) in enumerate(zip(work, route0)):
            whole, turned = scratch[2 * i], scratch[2 * i + 1]
            for k in range(4):
                row = pl.multiple_of(((x + k) % 4) * STRIP, 16)
                whole[pl.ds(row, STRIP), :] = (
                    pair[:, columns(j)] if k == 0 else rest[(k - 1) * STRIP : k * STRIP, :]
                )
            column = pl.multiple_of(((y + step + 4) % 4) * GROUP, 128)
            for name, first, at, width in ROUTE0[j]:
                turned[at : at + width, :] = whole[:, at : at + width].T
                start(
                    turned.at[pl.ds(at, width), :],
                    outs[name].at[pl.ds(first, width), pl.ds(column, GROUP)],
                )
        for copy in started:
            copy.wait()

    n = len(work)
    own, partner = list(zip(units[:n], units[n : 2 * n])), list(zip(units[2 * n : 3 * n], units[3 * n :]))

    @pl.when(c == 0)
    def _():
        lay(own, partner)

    @pl.when(c == 1)
    def _():
        lay(partner, own)


LAID = (
    ((0, 0), (0, 1), (0, 2)),
    ((-1, 0), (1, 1)),
    ((1, 0), (2, 0)),
    ((-1, 1), (2, 1), (1, 2)),
    ((-1, 2), (2, 2)),
)


def lay(work, mine, theirs, before):
    n = len(work)
    n_in = 0 if before is None else 3
    shapes = tuple(jax.ShapeDtypeStruct(SHAPES[name], jnp.bfloat16) for name in NAMES)
    units = [u[s][at(j)] for u in (mine, theirs) for at in (lambda j: 3, lambda j: j) for s, j in work]
    return pl.pallas_call(
        lambda *refs: lay_kernel(work, n_in, *refs),
        out_shape=shapes,
        in_specs=vmem(4 * n) + anywhere(n_in),
        out_specs=tuple(anywhere(3)),
        scratch_shapes=[
            pltpu.VMEM(shape, jnp.bfloat16)
            for _, j in work
            for shape in ((GROUP, WIDTHS[j]), (WIDTHS[j], GROUP))
        ]
        + [pltpu.SemaphoreType.DMA((6 * n,))],
        input_output_aliases={4 * n + i: i for i in range(n_in)},
        compiler_params=pltpu.CompilerParams(vmem_limit_bytes=10 * 2**20),
    )(*held(units), *(before or ()))


STEPS = (0, -1, 1, 2)


def value_kernel(*refs):
    units, out, whole, turned, sems = refs[:16], refs[16], refs[17], refs[18], refs[19]
    y, x, c = place()

    def gather(pairs, rests):
        for step, pair, rest in zip(STEPS, pairs, rests):
            g = (x + step + 4) % 4
            for k in range(4):
                row = pl.multiple_of(((y + k) % 4) * GROUP + g * STRIP, 16)
                whole[pl.ds(row, STRIP), :] = (
                    pair[:, columns(0)] if k == 0 else rest[(k - 1) * STRIP : k * STRIP, :]
                )

    @pl.when(c == 0)
    def _():
        gather(units[8:12], units[12:])

    @pl.when(c == 1)
    def _():
        gather(units[:4], units[4:8])

    copies = []
    for s in range(4):
        turned[s] = whole[s * GROUP : (s + 1) * GROUP, :].T
        copy = pltpu.make_async_copy(turned.at[s], out.at[:, pl.ds(s * GROUP, GROUP)], sems.at[s])
        copy.start()
        copies.append(copy)
    for copy in copies:
        copy.wait()


def value_of(units):
    return pl.pallas_call(
        value_kernel,
        out_shape=jax.ShapeDtypeStruct((512, 3584), jnp.bfloat16),
        in_specs=vmem(16),
        out_specs=pl.BlockSpec(memory_space=pl.ANY),
        scratch_shapes=[
            pltpu.VMEM((3584, 512), jnp.bfloat16),
            pltpu.VMEM((4, 512, GROUP), jnp.bfloat16),
            pltpu.SemaphoreType.DMA((4,)),
        ],
        compiler_params=pltpu.CompilerParams(vmem_limit_bytes=10 * 2**20),
        name="value",
    )(*held(units))


def join_kernel(here, there, out):
    rows = out.shape[0]
    mine = here[0:rows, :].astype(jnp.float32)
    out[...] = jnp.where(mine != 0, mine, there[0:rows, :].astype(jnp.float32)).astype(out.dtype)


def join(here, there, out):
    return pl.pallas_call(
        join_kernel,
        out_shape=out,
        in_specs=vmem(2),
        out_specs=pl.BlockSpec(memory_space=pltpu.VMEM),
        compiler_params=pltpu.CompilerParams(vmem_limit_bytes=2 * 2**20),
    )(*held((here, there)))


NEAR, ACROSS = (1, 0, 3, 2), (3, 2, 1, 0)


def along_first(partners):
    return pairs(lambda y, x, c: (y, partners[x], c) if c == 0 else (partners[y], x, c))


def meet(norm):
    route = (along_first(NEAR), along_first(ACROSS), PARTNER)
    moves = [("width", list(enumerate(NEAR))), ("width", list(enumerate(ACROSS)))]
    moves += [(ZERO, move) for move in route + route]
    for k, (axis, move) in enumerate(moves):
        there = lax.ppermute(norm, axis, move)
        last = k + 1 == len(moves)
        out = jax.ShapeDtypeStruct((28, 128), norm.dtype) if last else pltpu.VMEM((32, 128), norm.dtype)
        norm = join(norm, there, out)
    return norm.reshape(-1)


def body(
    train_query,
    low_query,
    high_query,
    train_key,
    low_key,
    high_key,
    train_value,
    low_value,
    high_value,
    train_mixed,
    low_mixed,
    high_mixed,
    norm_train,
    norm_step,
):
    keep, give, norm = merge(
        train_query,
        low_query.T,
        high_query,
        train_key,
        low_key.T,
        high_key,
        train_value,
        low_value.T,
        high_value,
        train_mixed.T,
        high_mixed,
        low_mixed.T,
        norm_train.reshape(1, NORM),
        norm_step.reshape(1, NORM),
    )
    beside = send(give, PARTNER)
    keep_up = send(keep, first_axis(1))
    give_down = send(give, first_axis_across(-1))
    keep_down = send(keep, first_axis(-1))
    give_up = send(give, first_axis_across(1))
    far_keep = send(keep_up, first_axis(1))
    far_give = send(give_down, first_axis(-1))
    pair = pair_of(keep, beside)
    rest = stack((keep_up, keep_down, give_up, give_down, far_keep, far_give))
    units = (*rest, pair)
    mine = {
        0: units,
        -1: [send(u, second_axis(1)) for u in units],
        1: [send(u, second_axis(-1)) for u in units],
    }
    mine[2] = [
        send(mine[-1][j], second_axis(1))
        if j in (0, 3)
        else send(mine[1][j], second_axis(-1))
        for j in range(4)
    ]
    theirs = {s: [send(u, PARTNER) for u in mine[s]] for s in STEPS}

    outs = None
    for work in LAID:
        outs = lay(work, mine, theirs, outs)
    ready_query, ready_key, ready_mixed = outs
    ready_value = value_of([u[s][j] for u in (mine, theirs) for j in (3, 0) for s in STEPS])

    serve_norm = meet(norm)
    return (ready_query, ready_key, ready_value, ready_mixed, serve_norm)


def solution(mesh):
    torus = Mesh(
        mesh.devices.reshape(4, 4, 2, mesh.shape["width"]), ("zero_0", "zero_1", "zero_2", "width")
    )
    return jax.shard_map(
        body,
        mesh=torus,
        in_specs=(
            P(ZERO, "width"),
            P(ZERO, None),
            P(None, "width"),
            P(ZERO, "width"),
            P(ZERO, None),
            P(None, "width"),
            P(ZERO, "width"),
            P(ZERO, None),
            P(None, "width"),
            P("width", ZERO),
            P("width", None),
            P(None, ZERO),
            P(ZERO_WIDTH),
            P(ZERO_WIDTH),
        ),
        out_specs=(P("width", None), P("width", None), P("width", None), P(None, "width"), P()),
        check_vma=False,
    )
```

```python
import jax
import jax.numpy as jnp
from jax import lax
from jax.experimental import pallas as pl
from jax.experimental.pallas import tpu as pltpu
from jax.sharding import Mesh
from jax.sharding import PartitionSpec as P

ZERO = ("zero_0", "zero_1", "zero_2")
ZERO_WIDTH = ("zero_0", "zero_1", "zero_2", "width")


mix_rate = 0.5

ROWS = 112
HALF = 1536
CHUNK = 512
GROUP = 8 * ROWS
STRIP = 2 * ROWS
REST = 3 * STRIP
NORM = 28
TILE = (8, 512)

ROUTE0 = (("query", 0), ("query", 512), ("key", 0))
ROUTE1 = (("value", 0), ("mixed", 0), ("mixed", 512))

UNITS_OF = ((3, 0, 2), (3, 1), (3, 2))


def spot(j, k):
    if k == 0:
        return 3, 0, j * CHUNK
    if j == 0:
        return (2, REST, 0) if k == 2 else (0, (k - 1) // 2 * STRIP, 0)
    return j, (k - 1) * STRIP, 0


def pairs(move):
    return [
        ((y * 4 + x) * 2 + c, ((v % 4) * 4 + u % 4) * 2 + d)
        for y in range(4)
        for x in range(4)
        for c in range(2)
        for v, u, d in (move(y, x, c),)
    ]


def first_axis(step):
    return pairs(lambda y, x, c: (y, x + step, c) if c == 0 else (y + step, x, c))


def first_axis_across(step):
    return pairs(lambda y, x, c: (y, x + step, 0) if c == 1 else (y + step, x, 1))


def second_axis(step):
    return pairs(lambda y, x, c: (y + step, x, c) if c == 0 else (y, x + step, c))


PARTNER = pairs(lambda y, x, c: (y, x, 1 - c))


def send(array, to):
    return lax.ppermute(array, ZERO, to)


def place():
    return tuple(lax.axis_index(a) for a in ZERO)


def held(arrays):
    return [pltpu.with_memory_space_constraint(a, pltpu.VMEM) for a in arrays]


def vmem(n):
    return [pl.BlockSpec(memory_space=pltpu.VMEM)] * n


def anywhere(n):
    return [pl.BlockSpec(memory_space=pl.ANY)] * n


MERGED = (
    (ROWS, 1024), (32, ROWS), (32, 1024),
    (ROWS, 512), (32, ROWS), (32, 512),
    (ROWS, 512), (32, ROWS), (32, 512),
    (ROWS, 1024), (32, ROWS), (32, 1024),
    (1, NORM), (1, NORM),
)


def merge_kernel(*refs):
    ins, (keep, give), here, (line, sems) = refs[:14], refs[14:16], refs[16:30], refs[30:]
    y, x, c = place()
    copies = [pltpu.make_async_copy(a, b, sems.at[i]) for i, (a, b) in enumerate(zip(ins, here))]
    for copy in copies:
        copy.start()
    line[...] = jnp.zeros(line.shape, jnp.float32)
    for copy in copies:
        copy.wait()
    tq, lq, hq, tk, lk, hk, tv, lv, hv, tm, lm, hm, gain, step = here

    def latest(train, low, high):
        product = lax.dot_general(
            low[...], high[...], (((0,), (0,)), ((), ())), preferred_element_type=jnp.float32
        )
        return (train[...].astype(jnp.float32) + mix_rate * product).astype(jnp.bfloat16)

    first = ((((y * 4 + x) * 2 + c) * 4) + lax.axis_index("width")) * NORM
    row, at = first // 512, first % 512
    lane = lax.broadcasted_iota(jnp.int32, (1, 512), 1)
    line[0:1, 0:NORM] = gain[...] + step[...]
    turned = pltpu.roll(line[0:1, :], at, 1)
    line[0:1, :] = jnp.zeros((1, 512), jnp.float32)
    line[pl.ds(row, 1), :] = jnp.where(lane >= at, turned, 0.0)
    line[pl.ds(row + 1, 1), :] = jnp.where(lane < at, turned, line[pl.ds(row + 1, 1), :])
    for to in (keep, give):
        to[ROWS : ROWS + 8, 0:512] = line[...].astype(jnp.bfloat16)

    rows = slice(0, ROWS)

    def fill(first, second):
        first[rows, 0:1024] = latest(tq, lq, hq)
        first[rows, 1024:1536] = latest(tk, lk, hk)
        second[rows, 0:512] = latest(tv, lv, hv)
        second[rows, 512:1536] = latest(tm, lm, hm)

    @pl.when(c == 0)
    def _():
        fill(keep, give)

    @pl.when(c == 1)
    def _():
        fill(give, keep)


def merge(*args):
    piece = pltpu.VMEM((ROWS + 8, HALF), jnp.bfloat16)
    return pl.pallas_call(
        merge_kernel,
        out_shape=(piece, piece),
        in_specs=anywhere(len(args)),
        out_specs=tuple(vmem(2)),
        scratch_shapes=[pltpu.VMEM(shape, a.dtype) for shape, a in zip(MERGED, args)]
        + [pltpu.VMEM(TILE, jnp.float32), pltpu.SemaphoreType.DMA((14,))],
        compiler_params=pltpu.CompilerParams(vmem_limit_bytes=8 * 2**20),
        name="merge",
    )(*[pltpu.with_memory_space_constraint(a, pltpu.HBM) for a in args])


def pair_kernel(keep, beside, out):
    _, _, c = place()
    for piece, core in ((keep, c), (beside, 1 - c)):
        out[pl.ds(pl.multiple_of(core * ROWS, 16), ROWS), :] = piece[0:ROWS, :]


def pair_of(keep, beside):
    return pl.pallas_call(
        pair_kernel,
        out_shape=pltpu.VMEM((STRIP, HALF), jnp.bfloat16),
        in_specs=vmem(2),
        out_specs=pl.BlockSpec(memory_space=pltpu.VMEM),
        compiler_params=pltpu.CompilerParams(vmem_limit_bytes=2 * 2**20),
        name="pair",
    )(*held((keep, beside)))


OFFSETS = ((3, 0), (1, 0), (3, 1), (1, 1), (2, 0), (2, 1))


def place_pieces(pieces, units, spots):
    _, _, c = place()
    for piece, (k, other) in zip(pieces, OFFSETS):
        core = c if other == 0 else 1 - c
        for j in range(3):
            if (j, k) in spots:
                unit, row, _ = spot(j, k)
                at = pl.multiple_of(row + core * ROWS, 16)
                units[unit][pl.ds(at, ROWS), :] = piece[0:ROWS, j * CHUNK : (j + 1) * CHUNK]


def near_kernel(*refs):
    place_pieces(refs[:4], {0: refs[4]}, ((0, 1), (0, 3)))


def known(*tiles):
    found = tiles[0].astype(jnp.float32)
    for tile in tiles[1:]:
        found = jnp.where(found != 0, found, tile.astype(jnp.float32))
    return found


def rest_kernel(*refs):
    pieces, one, two, tile = refs[:8], refs[8], refs[9], refs[10]
    spots = [(j, k) for j in (1, 2) for k in (1, 2, 3)] + [(0, 2)]
    place_pieces(pieces[:6], {1: one, 2: two}, spots)
    tile[...] = known(*[p[ROWS : ROWS + 8, 0:512] for p in pieces]).astype(tile.dtype)


def stack(kernel, pieces, shapes):
    return pl.pallas_call(
        kernel,
        out_shape=tuple(pltpu.VMEM(shape, jnp.bfloat16) for shape in shapes),
        in_specs=vmem(len(pieces)),
        out_specs=tuple(vmem(len(shapes))),
        compiler_params=pltpu.CompilerParams(vmem_limit_bytes=4 * 2**20),
    )(*held(pieces))


NAMES = ("query", "key", "mixed")
SHAPES = {"query": (1024, 3584), "key": (512, 3584), "mixed": (3584, 1024)}


def lay_kernel(work, keys, n_in, *refs):
    n = len(keys)
    own, partner, refs = dict(zip(keys, refs)), dict(zip(keys, refs[n:])), refs[2 * n + n_in :]
    outs, (whole, turned, sems) = dict(zip(NAMES, refs[:3])), refs[3:]
    y, x, c = place()

    def lay(route0, route1):
        started = []

        def start(source, target):
            copy = pltpu.make_async_copy(source, target, sems.at[len(started)])
            copy.start()
            started.append(copy)

        for step, j in work:
            name, first = ROUTE1[j]
            if name == "mixed":
                g = (x + step + 4) % 4
                for k in range(4):
                    row = pl.multiple_of(((y + k) % 4) * GROUP + g * STRIP, 16)
                    unit, at, column = spot(j, k)
                    start(
                        route1[step, unit].at[pl.ds(at, STRIP), pl.ds(column, CHUNK)],
                        outs[name].at[pl.ds(row, STRIP), pl.ds(first, CHUNK)],
                    )
        for i, (step, j) in enumerate(work):
            name, first = ROUTE0[j]
            for k in range(4):
                row = pl.multiple_of(((x + k) % 4) * STRIP, 16)
                unit, at, column = spot(j, k)
                whole[i, pl.ds(row, STRIP), :] = route0[step, unit][
                    at : at + STRIP, column : column + CHUNK
                ]
            turned[i] = whole[i].T
            column = pl.multiple_of(((y + step + 4) % 4) * GROUP, 128)
            start(turned.at[i], outs[name].at[pl.ds(first, CHUNK), pl.ds(column, GROUP)])
        for copy in started:
            copy.wait()

    @pl.when(c == 0)
    def _():
        lay(own, partner)

    @pl.when(c == 1)
    def _():
        lay(partner, own)


LAID = (
    ((0, 0), (0, 1), (0, 2)),
    ((-1, 0), (-1, 2), (1, 1)),
    ((1, 0), (1, 2)),
    ((2, 0), (2, 2)),
    ((-1, 1), (2, 1)),
)


def lay(work, mine, theirs, before):
    n = len(work)
    n_in = 0 if before is None else 3
    shapes = tuple(jax.ShapeDtypeStruct(SHAPES[name], jnp.bfloat16) for name in NAMES)
    keys = tuple(dict.fromkeys((s, u) for s, j in work for u in UNITS_OF[j]))
    units = [side[s][u] for side in (mine, theirs) for s, u in keys]
    return pl.pallas_call(
        lambda *refs: lay_kernel(work, keys, n_in, *refs),
        out_shape=shapes,
        in_specs=vmem(len(units)) + anywhere(n_in),
        out_specs=tuple(anywhere(3)),
        scratch_shapes=[
            pltpu.VMEM((n, GROUP, CHUNK), jnp.bfloat16),
            pltpu.VMEM((n, CHUNK, GROUP), jnp.bfloat16),
            pltpu.SemaphoreType.DMA((5 * n,)),
        ],
        input_output_aliases={len(units) + i: i for i in range(n_in)},
        compiler_params=pltpu.CompilerParams(vmem_limit_bytes=10 * 2**20),
    )(*held(units), *(before or ()))


STEPS = (0, -1, 1, 2)
VALUE_KEYS = tuple((s, u) for s in STEPS for u in UNITS_OF[0])


def value_kernel(*refs):
    n = len(VALUE_KEYS)
    own, partner, refs = dict(zip(VALUE_KEYS, refs)), dict(zip(VALUE_KEYS, refs[n:])), refs[2 * n :]
    out, whole, turned, sems = refs
    y, x, c = place()

    def gather(route1):
        for step in STEPS:
            g = (x + step + 4) % 4
            for k in range(4):
                row = pl.multiple_of(((y + k) % 4) * GROUP + g * STRIP, 16)
                unit, at, column = spot(0, k)
                whole[pl.ds(row, STRIP), :] = route1[step, unit][
                    at : at + STRIP, column : column + CHUNK
                ]

    @pl.when(c == 0)
    def _():
        gather(partner)

    @pl.when(c == 1)
    def _():
        gather(own)

    copies = []
    for s in range(4):
        turned[s] = whole[s * GROUP : (s + 1) * GROUP, :].T
        copy = pltpu.make_async_copy(turned.at[s], out.at[:, pl.ds(s * GROUP, GROUP)], sems.at[s])
        copy.start()
        copies.append(copy)
    for copy in copies:
        copy.wait()


def value_of(units):
    return pl.pallas_call(
        value_kernel,
        out_shape=jax.ShapeDtypeStruct((512, 3584), jnp.bfloat16),
        in_specs=vmem(2 * len(VALUE_KEYS)),
        out_specs=pl.BlockSpec(memory_space=pl.ANY),
        scratch_shapes=[
            pltpu.VMEM((3584, 512), jnp.bfloat16),
            pltpu.VMEM((4, 512, GROUP), jnp.bfloat16),
            pltpu.SemaphoreType.DMA((4,)),
        ],
        compiler_params=pltpu.CompilerParams(vmem_limit_bytes=10 * 2**20),
        name="value",
    )(*held(units))


def join_kernel(here, there, out):
    out[...] = known(here[...], there[...]).astype(jnp.bfloat16)


def norm_kernel(here, there, out, rows):
    found = known(here[...], there[...])
    for r in range(28):
        rows[r : r + 1, :] = found[r // 4 : r // 4 + 1, r % 4 * 128 : (r % 4 + 1) * 128]
    out[...] = rows[0:28, :].astype(jnp.bfloat16)


NEAR, ACROSS = (1, 0, 3, 2), (3, 2, 1, 0)


def along_first(partners):
    return pairs(lambda y, x, c: (y, partners[x], c) if c == 0 else (partners[y], x, c))


def norm_of(tile):
    moves = (
        (ZERO, PARTNER), (ZERO, along_first(NEAR)), (ZERO, along_first(ACROSS)),
        ("width", list(enumerate(NEAR))), ("width", list(enumerate(ACROSS))),
    )
    for k, (axis, move) in enumerate(moves):
        there = lax.ppermute(tile, axis, move)
        if k < 4:
            (tile,) = stack(join_kernel, (tile, there), (TILE,))
    return pl.pallas_call(
        norm_kernel,
        out_shape=jax.ShapeDtypeStruct((28, 128), jnp.bfloat16),
        in_specs=vmem(2),
        out_specs=pl.BlockSpec(memory_space=pltpu.VMEM),
        scratch_shapes=[pltpu.VMEM((32, 128), jnp.float32)],
        compiler_params=pltpu.CompilerParams(vmem_limit_bytes=2 * 2**20),
        name="norm",
    )(*held((tile, there))).reshape(-1)


def body(
    train_query,
    low_query,
    high_query,
    train_key,
    low_key,
    high_key,
    train_value,
    low_value,
    high_value,
    train_mixed,
    low_mixed,
    high_mixed,
    norm_train,
    norm_step,
):
    keep, give = merge(
        train_query,
        low_query.T,
        high_query,
        train_key,
        low_key.T,
        high_key,
        train_value,
        low_value.T,
        high_value,
        train_mixed.T,
        high_mixed,
        low_mixed.T,
        norm_train.reshape(1, NORM),
        norm_step.reshape(1, NORM),
    )
    beside = send(give, PARTNER)
    keep_up = send(keep, first_axis(1))
    give_down = send(give, first_axis_across(-1))
    keep_down = send(keep, first_axis(-1))
    give_up = send(give, first_axis_across(1))
    far_keep = send(keep_up, first_axis(1))
    far_give = send(give_down, first_axis(-1))
    pieces = (keep_up, keep_down, give_up, give_down, far_keep, far_give)
    (near,) = stack(near_kernel, pieces[:4], ((2 * STRIP, CHUNK),))
    shapes = ((REST, CHUNK), (REST + STRIP, CHUNK), TILE)
    *rest, tile = stack(rest_kernel, (*pieces, keep, beside), shapes)
    units = (near, *rest, pair_of(keep, beside))
    mine = {
        0: units,
        -1: [send(u, second_axis(1)) for u in units],
        1: [send(u, second_axis(-1)) for u in units],
    }
    mine[2] = [
        send(mine[-1][j], second_axis(1))
        if j in (0, 2)
        else send(mine[1][j], second_axis(-1))
        for j in range(4)
    ]
    theirs = {s: [send(u, PARTNER) for u in mine[s]] for s in STEPS}

    outs = None
    for work in LAID:
        outs = lay(work, mine, theirs, outs)
    ready_query, ready_key, ready_mixed = outs
    ready_value = value_of([side[s][u] for side in (mine, theirs) for s, u in VALUE_KEYS])

    serve_norm = norm_of(tile)
    return (ready_query, ready_key, ready_value, ready_mixed, serve_norm)


def solution(mesh):
    torus = Mesh(
        mesh.devices.reshape(4, 4, 2, mesh.shape["width"]), ("zero_0", "zero_1", "zero_2", "width")
    )
    return jax.shard_map(
        body,
        mesh=torus,
        in_specs=(
            P(ZERO, "width"),
            P(ZERO, None),
            P(None, "width"),
            P(ZERO, "width"),
            P(ZERO, None),
            P(None, "width"),
            P(ZERO, "width"),
            P(ZERO, None),
            P(None, "width"),
            P("width", ZERO),
            P("width", None),
            P(None, ZERO),
            P(ZERO_WIDTH),
            P(ZERO_WIDTH),
        ),
        out_specs=(P("width", None), P("width", None), P("width", None), P(None, "width"), P()),
        check_vma=False,
    )
```

```python
import jax
import jax.numpy as jnp
from jax import lax
from jax.experimental import pallas as pl
from jax.experimental.pallas import tpu as pltpu
from jax.sharding import Mesh
from jax.sharding import PartitionSpec as P

ZERO = ("zero_0", "zero_1", "zero_2")
ZERO_WIDTH = ("zero_0", "zero_1", "zero_2", "width")


mix_rate = 0.5

ROWS = 112
HALF = 1536
CHUNK = 512
PART = 128
GROUP = 8 * ROWS
STRIP = 2 * ROWS
REST = 3 * STRIP
NORM = 28
TILE = (8, 512)

ROUTE0 = (("query", 0), ("query", 512), ("key", 0))
ROUTE1 = (("value", 0), ("mixed", 0), ("mixed", 512))

UNITS_OF = ((3, 0, 2), (3, 1), (3, 2))


def spot(j, k):
    if k == 0:
        return 3, 0, j * CHUNK
    if j == 0:
        return (2, REST, 0) if k == 2 else (0, (k - 1) // 2 * STRIP, 0)
    return j, (k - 1) * STRIP, 0


def pairs(move):
    return [
        ((y * 4 + x) * 2 + c, ((v % 4) * 4 + u % 4) * 2 + d)
        for y in range(4)
        for x in range(4)
        for c in range(2)
        for v, u, d in (move(y, x, c),)
    ]


def first_axis(step):
    return pairs(lambda y, x, c: (y, x + step, c) if c == 0 else (y + step, x, c))


def first_axis_across(step):
    return pairs(lambda y, x, c: (y, x + step, 0) if c == 1 else (y + step, x, 1))


def second_axis(step):
    return pairs(lambda y, x, c: (y + step, x, c) if c == 0 else (y, x + step, c))


PARTNER = pairs(lambda y, x, c: (y, x, 1 - c))


def send(array, to):
    return lax.ppermute(array, ZERO, to)


def place():
    return tuple(lax.axis_index(a) for a in ZERO)


def held(arrays):
    return [pltpu.with_memory_space_constraint(a, pltpu.VMEM) for a in arrays]


def vmem(n):
    return [pl.BlockSpec(memory_space=pltpu.VMEM)] * n


def anywhere(n):
    return [pl.BlockSpec(memory_space=pl.ANY)] * n


MERGED = (
    (ROWS, 1024), (32, ROWS), (32, 1024),
    (ROWS, 512), (32, ROWS), (32, 512),
    (ROWS, 512), (32, ROWS), (32, 512),
    (ROWS, 1024), (32, ROWS), (32, 1024),
    (1, NORM), (1, NORM),
)


def merge_kernel(*refs):
    ins, (keep, give), here, (line, sems) = refs[:14], refs[14:16], refs[16:30], refs[30:]
    y, x, c = place()
    copies = [pltpu.make_async_copy(a, b, sems.at[i]) for i, (a, b) in enumerate(zip(ins, here))]
    for copy in copies:
        copy.start()
    line[...] = jnp.zeros(line.shape, jnp.float32)
    for copy in copies:
        copy.wait()
    tq, lq, hq, tk, lk, hk, tv, lv, hv, tm, lm, hm, gain, step = here

    def latest(train, low, high):
        product = lax.dot_general(
            low[...], high[...], (((0,), (0,)), ((), ())), preferred_element_type=jnp.float32
        )
        return (train[...].astype(jnp.float32) + mix_rate * product).astype(jnp.bfloat16)

    first = ((((y * 4 + x) * 2 + c) * 4) + lax.axis_index("width")) * NORM
    row, at = first // 512, first % 512
    lane = lax.broadcasted_iota(jnp.int32, (1, 512), 1)
    line[0:1, 0:NORM] = gain[...] + step[...]
    turned = pltpu.roll(line[0:1, :], at, 1)
    line[0:1, :] = jnp.zeros((1, 512), jnp.float32)
    line[pl.ds(row, 1), :] = jnp.where(lane >= at, turned, 0.0)
    line[pl.ds(row + 1, 1), :] = jnp.where(lane < at, turned, line[pl.ds(row + 1, 1), :])
    for to in (keep, give):
        to[ROWS : ROWS + 8, 0:512] = line[...].astype(jnp.bfloat16)

    rows = slice(0, ROWS)

    def fill(first, second):
        first[rows, 0:1024] = latest(tq, lq, hq)
        first[rows, 1024:1536] = latest(tk, lk, hk)
        second[rows, 0:512] = latest(tv, lv, hv)
        second[rows, 512:1536] = latest(tm, lm, hm)

    @pl.when(c == 0)
    def _():
        fill(keep, give)

    @pl.when(c == 1)
    def _():
        fill(give, keep)


def merge(*args):
    piece = pltpu.VMEM((ROWS + 8, HALF), jnp.bfloat16)
    return pl.pallas_call(
        merge_kernel,
        out_shape=(piece, piece),
        in_specs=anywhere(len(args)),
        out_specs=tuple(vmem(2)),
        scratch_shapes=[pltpu.VMEM(shape, a.dtype) for shape, a in zip(MERGED, args)]
        + [pltpu.VMEM(TILE, jnp.float32), pltpu.SemaphoreType.DMA((14,))],
        compiler_params=pltpu.CompilerParams(vmem_limit_bytes=8 * 2**20),
        name="merge",
    )(*[pltpu.with_memory_space_constraint(a, pltpu.HBM) for a in args])


def pair_kernel(keep, beside, out):
    _, _, c = place()
    for piece, core in ((keep, c), (beside, 1 - c)):
        out[pl.ds(pl.multiple_of(core * ROWS, 16), ROWS), :] = piece[0:ROWS, :]


def pair_of(keep, beside):
    return pl.pallas_call(
        pair_kernel,
        out_shape=pltpu.VMEM((STRIP, HALF), jnp.bfloat16),
        in_specs=vmem(2),
        out_specs=pl.BlockSpec(memory_space=pltpu.VMEM),
        compiler_params=pltpu.CompilerParams(vmem_limit_bytes=2 * 2**20),
        name="pair",
    )(*held((keep, beside)))


OFFSETS = ((3, 0), (1, 0), (3, 1), (1, 1), (2, 0), (2, 1))


def place_pieces(pieces, units, spots):
    _, _, c = place()
    for piece, (k, other) in zip(pieces, OFFSETS):
        core = c if other == 0 else 1 - c
        for j in range(3):
            if (j, k) in spots:
                unit, row, _ = spot(j, k)
                at = pl.multiple_of(row + core * ROWS, 16)
                units[unit][pl.ds(at, ROWS), :] = piece[0:ROWS, j * CHUNK : (j + 1) * CHUNK]


def near_kernel(*refs):
    place_pieces(refs[:4], {0: refs[4]}, ((0, 1), (0, 3)))


def known(*tiles):
    found = tiles[0].astype(jnp.float32)
    for tile in tiles[1:]:
        found = jnp.where(found != 0, found, tile.astype(jnp.float32))
    return found


def rest_kernel(*refs):
    pieces, one, two, tile = refs[:8], refs[8], refs[9], refs[10]
    spots = [(j, k) for j in (1, 2) for k in (1, 2, 3)] + [(0, 2)]
    place_pieces(pieces[:6], {1: one, 2: two}, spots)
    tile[...] = known(*[p[ROWS : ROWS + 8, 0:512] for p in pieces]).astype(tile.dtype)


def stack(kernel, pieces, shapes):
    return pl.pallas_call(
        kernel,
        out_shape=tuple(pltpu.VMEM(shape, jnp.bfloat16) for shape in shapes),
        in_specs=vmem(len(pieces)),
        out_specs=tuple(vmem(len(shapes))),
        compiler_params=pltpu.CompilerParams(vmem_limit_bytes=4 * 2**20),
    )(*held(pieces))


NAMES = ("query", "key", "mixed")
SHAPES = {"query": (1024, 3584), "key": (512, 3584), "mixed": (3584, 1024)}


def lay_kernel(work, sides, keys, n_in, *refs):
    n = len(keys)
    units = {side: dict(zip(keys, refs[i * n :])) for i, side in enumerate(sides)}
    own, partner, refs = units.get("own"), units.get("partner"), refs[len(sides) * n + n_in :]
    outs, (whole, turned, sems) = dict(zip(NAMES, refs[:3])), refs[3:]
    y, x, c = place()

    def lay(route0, route1):
        started = []

        def start(source, target):
            copy = pltpu.make_async_copy(source, target, sems.at[len(started)])
            copy.start()
            started.append(copy)

        for step, j in work if route1 else ():
            name, first = ROUTE1[j]
            if name == "mixed":
                g = (x + step + 4) % 4
                for k in range(4):
                    row = pl.multiple_of(((y + k) % 4) * GROUP + g * STRIP, 16)
                    unit, at, column = spot(j, k)
                    start(
                        route1[step, unit].at[pl.ds(at, STRIP), pl.ds(column, CHUNK)],
                        outs[name].at[pl.ds(row, STRIP), pl.ds(first, CHUNK)],
                    )
        for i, (step, j) in enumerate(work if route0 else ()):
            name, first = ROUTE0[j]
            for k in range(4):
                row = pl.multiple_of(((x + k) % 4) * STRIP, 16)
                unit, at, column = spot(j, k)
                whole[i, pl.ds(row, STRIP), :] = route0[step, unit][
                    at : at + STRIP, column : column + CHUNK
                ]
            column = pl.multiple_of(((y + step + 4) % 4) * GROUP, 128)
            for at in range(0, CHUNK, PART):
                turned[i, at : at + PART, :] = whole[i, :, at : at + PART].T
                start(
                    turned.at[i, pl.ds(at, PART), :],
                    outs[name].at[pl.ds(first + at, PART), pl.ds(column, GROUP)],
                )
        for copy in started:
            copy.wait()

    @pl.when(c == 0)
    def _():
        lay(own, partner)

    @pl.when(c == 1)
    def _():
        lay(partner, own)


BOTH = ("own", "partner")
LAID = (
    (((0, 0), (0, 1), (0, 2)), BOTH),
    (((-1, 0), (-1, 2), (1, 1)), BOTH),
    (((1, 0), (1, 2)), BOTH),
    (((2, 0), (2, 2)), BOTH),
    (((-1, 1), (2, 1)), ("own",)),
    (((-1, 1),), ("partner",)),
    (((2, 1),), ("partner",)),
)


def lay(work, sides, mine, theirs, before):
    n = len(work)
    n_in = 0 if before is None else 3
    shapes = tuple(jax.ShapeDtypeStruct(SHAPES[name], jnp.bfloat16) for name in NAMES)
    keys = tuple(dict.fromkeys((s, u) for s, j in work for u in UNITS_OF[j]))
    by_side = {"own": mine, "partner": theirs}
    units = [by_side[side][s][u] for side in sides for s, u in keys]
    return pl.pallas_call(
        lambda *refs: lay_kernel(work, sides, keys, n_in, *refs),
        out_shape=shapes,
        in_specs=vmem(len(units)) + anywhere(n_in),
        out_specs=tuple(anywhere(3)),
        scratch_shapes=[
            pltpu.VMEM((n, GROUP, CHUNK), jnp.bfloat16),
            pltpu.VMEM((n, CHUNK, GROUP), jnp.bfloat16),
            pltpu.SemaphoreType.DMA((8 * n,)),
        ],
        input_output_aliases={len(units) + i: i for i in range(n_in)},
        compiler_params=pltpu.CompilerParams(vmem_limit_bytes=10 * 2**20),
    )(*held(units), *(before or ()))


STEPS = (0, -1, 1, 2)
VALUE_KEYS = tuple((s, u) for s in STEPS for u in UNITS_OF[0])


def value_kernel(*refs):
    n = len(VALUE_KEYS)
    own, partner, refs = dict(zip(VALUE_KEYS, refs)), dict(zip(VALUE_KEYS, refs[n:])), refs[2 * n :]
    out, whole, turned, sems = refs
    y, x, c = place()

    def gather(route1):
        for step in STEPS:
            g = (x + step + 4) % 4
            for k in range(4):
                row = pl.multiple_of(((y + k) % 4) * GROUP + g * STRIP, 16)
                unit, at, column = spot(0, k)
                whole[pl.ds(row, STRIP), :] = route1[step, unit][
                    at : at + STRIP, column : column + CHUNK
                ]

    @pl.when(c == 0)
    def _():
        gather(partner)

    @pl.when(c == 1)
    def _():
        gather(own)

    copies = []
    for s in range(4):
        turned[s] = whole[s * GROUP : (s + 1) * GROUP, :].T
        copy = pltpu.make_async_copy(turned.at[s], out.at[:, pl.ds(s * GROUP, GROUP)], sems.at[s])
        copy.start()
        copies.append(copy)
    for copy in copies:
        copy.wait()


def value_of(units):
    return pl.pallas_call(
        value_kernel,
        out_shape=jax.ShapeDtypeStruct((512, 3584), jnp.bfloat16),
        in_specs=vmem(2 * len(VALUE_KEYS)),
        out_specs=pl.BlockSpec(memory_space=pl.ANY),
        scratch_shapes=[
            pltpu.VMEM((3584, 512), jnp.bfloat16),
            pltpu.VMEM((4, 512, GROUP), jnp.bfloat16),
            pltpu.SemaphoreType.DMA((4,)),
        ],
        compiler_params=pltpu.CompilerParams(vmem_limit_bytes=10 * 2**20),
        name="value",
    )(*held(units))


def join_kernel(here, there, out):
    out[...] = known(here[...], there[...]).astype(jnp.bfloat16)


def norm_kernel(here, there, out, rows):
    found = known(here[...], there[...])
    for r in range(28):
        rows[r : r + 1, :] = found[r // 4 : r // 4 + 1, r % 4 * 128 : (r % 4 + 1) * 128]
    out[...] = rows[0:28, :].astype(jnp.bfloat16)


NEAR, ACROSS = (1, 0, 3, 2), (3, 2, 1, 0)


def along_first(partners):
    return pairs(lambda y, x, c: (y, partners[x], c) if c == 0 else (partners[y], x, c))


def norm_of(tile):
    moves = (
        ("width", list(enumerate(ACROSS))), ("width", list(enumerate(NEAR))),
        (ZERO, PARTNER), (ZERO, along_first(NEAR)), (ZERO, along_first(ACROSS)),
    )
    for k, (axis, move) in enumerate(moves):
        there = lax.ppermute(tile, axis, move)
        if k < 4:
            (tile,) = stack(join_kernel, (tile, there), (TILE,))
    return pl.pallas_call(
        norm_kernel,
        out_shape=jax.ShapeDtypeStruct((28, 128), jnp.bfloat16),
        in_specs=vmem(2),
        out_specs=pl.BlockSpec(memory_space=pltpu.VMEM),
        scratch_shapes=[pltpu.VMEM((32, 128), jnp.float32)],
        compiler_params=pltpu.CompilerParams(vmem_limit_bytes=2 * 2**20),
        name="norm",
    )(*held((tile, there))).reshape(-1)


def body(
    train_query,
    low_query,
    high_query,
    train_key,
    low_key,
    high_key,
    train_value,
    low_value,
    high_value,
    train_mixed,
    low_mixed,
    high_mixed,
    norm_train,
    norm_step,
):
    keep, give = merge(
        train_query,
        low_query.T,
        high_query,
        train_key,
        low_key.T,
        high_key,
        train_value,
        low_value.T,
        high_value,
        train_mixed.T,
        high_mixed,
        low_mixed.T,
        norm_train.reshape(1, NORM),
        norm_step.reshape(1, NORM),
    )
    beside = send(give, PARTNER)
    keep_up = send(keep, first_axis(1))
    give_down = send(give, first_axis_across(-1))
    keep_down = send(keep, first_axis(-1))
    give_up = send(give, first_axis_across(1))
    far_keep = send(keep_up, first_axis(1))
    far_give = send(give_down, first_axis(-1))
    pieces = (keep_up, keep_down, give_up, give_down, far_keep, far_give)
    (near,) = stack(near_kernel, pieces[:4], ((2 * STRIP, CHUNK),))
    shapes = ((REST, CHUNK), (REST + STRIP, CHUNK), TILE)
    *rest, tile = stack(rest_kernel, (*pieces, keep, beside), shapes)
    units = (near, *rest, pair_of(keep, beside))
    mine = {
        0: units,
        -1: [send(u, second_axis(1)) for u in units],
        1: [send(u, second_axis(-1)) for u in units],
    }
    mine[2] = [
        send(mine[-1][j], second_axis(1))
        if j in (0, 2)
        else send(mine[1][j], second_axis(-1))
        for j in range(4)
    ]
    theirs = {s: [send(u, PARTNER) for u in mine[s]] for s in STEPS}

    outs = None
    for work, sides in LAID:
        outs = lay(work, sides, mine, theirs, outs)
    ready_query, ready_key, ready_mixed = outs
    ready_value = value_of([side[s][u] for side in (mine, theirs) for s, u in VALUE_KEYS])

    serve_norm = norm_of(tile)
    return (ready_query, ready_key, ready_value, ready_mixed, serve_norm)


def solution(mesh):
    torus = Mesh(
        mesh.devices.reshape(4, 4, 2, mesh.shape["width"]), ("zero_0", "zero_1", "zero_2", "width")
    )
    return jax.shard_map(
        body,
        mesh=torus,
        in_specs=(
            P(ZERO, "width"),
            P(ZERO, None),
            P(None, "width"),
            P(ZERO, "width"),
            P(ZERO, None),
            P(None, "width"),
            P(ZERO, "width"),
            P(ZERO, None),
            P(None, "width"),
            P("width", ZERO),
            P("width", None),
            P(None, ZERO),
            P(ZERO_WIDTH),
            P(ZERO_WIDTH),
        ),
        out_specs=(P("width", None), P("width", None), P("width", None), P(None, "width"), P()),
        check_vma=False,
    )
```

```python
import jax
import jax.numpy as jnp
from jax import lax
from jax.experimental import pallas as pl
from jax.experimental.pallas import tpu as pltpu
from jax.sharding import Mesh
from jax.sharding import PartitionSpec as P

ZERO = ("zero_0", "zero_1", "zero_2")
ZERO_WIDTH = ("zero_0", "zero_1", "zero_2", "width")


mix_rate = 0.5

ROWS = 112
HALF = 1536
CHUNK = 512
PART = 128
GROUP = 8 * ROWS
STRIP = 2 * ROWS
REST = 3 * STRIP
NORM = 28
TILE = (8, 512)

ROUTE0 = (("query", 0), ("query", 512), ("key", 0))
ROUTE1 = (("value", 0), ("mixed", 0), ("mixed", 512))

UNITS_OF = ((3, 0, 2), (3, 1), (3, 2))


def spot(j, k):
    if k == 0:
        return 3, 0, j * CHUNK
    if j == 0:
        return (2, REST, 0) if k == 2 else (0, (k - 1) // 2 * STRIP, 0)
    return j, (k - 1) * STRIP, 0


def pairs(move):
    return [
        ((y * 4 + x) * 2 + c, ((v % 4) * 4 + u % 4) * 2 + d)
        for y in range(4)
        for x in range(4)
        for c in range(2)
        for v, u, d in (move(y, x, c),)
    ]


def first_axis(step):
    return pairs(lambda y, x, c: (y, x + step, c) if c == 0 else (y + step, x, c))


def first_axis_across(step):
    return pairs(lambda y, x, c: (y, x + step, 0) if c == 1 else (y + step, x, 1))


def second_axis(step):
    return pairs(lambda y, x, c: (y + step, x, c) if c == 0 else (y, x + step, c))


PARTNER = pairs(lambda y, x, c: (y, x, 1 - c))


def send(array, to):
    return lax.ppermute(array, ZERO, to)


def place():
    return tuple(lax.axis_index(a) for a in ZERO)


def held(arrays):
    return [pltpu.with_memory_space_constraint(a, pltpu.VMEM) for a in arrays]


def vmem(n):
    return [pl.BlockSpec(memory_space=pltpu.VMEM)] * n


def anywhere(n):
    return [pl.BlockSpec(memory_space=pl.ANY)] * n


MERGED = (
    (ROWS, 1024), (32, ROWS), (32, 1024),
    (ROWS, 512), (32, ROWS), (32, 512),
    (ROWS, 512), (32, ROWS), (32, 512),
    (ROWS, 1024), (32, ROWS), (32, 1024),
    (1, NORM), (1, NORM),
)


def merge_kernel(*refs):
    ins, (keep, give), here, (line, sems) = refs[:14], refs[14:16], refs[16:30], refs[30:]
    y, x, c = place()
    copies = [pltpu.make_async_copy(a, b, sems.at[i]) for i, (a, b) in enumerate(zip(ins, here))]
    for copy in copies[12:] + copies[:12]:
        copy.start()
    line[...] = jnp.zeros(line.shape, jnp.float32)
    for copy in copies[12:]:
        copy.wait()
    tq, lq, hq, tk, lk, hk, tv, lv, hv, tm, lm, hm, gain, step = here

    def latest(train, low, high):
        product = lax.dot_general(
            low[...], high[...], (((0,), (0,)), ((), ())), preferred_element_type=jnp.float32
        )
        return (train[...].astype(jnp.float32) + mix_rate * product).astype(jnp.bfloat16)

    first = ((((y * 4 + x) * 2 + c) * 4) + lax.axis_index("width")) * NORM
    row, at = first // 512, first % 512
    lane = lax.broadcasted_iota(jnp.int32, (1, 512), 1)
    line[0:1, 0:NORM] = gain[...] + step[...]
    turned = pltpu.roll(line[0:1, :], at, 1)
    line[0:1, :] = jnp.zeros((1, 512), jnp.float32)
    line[pl.ds(row, 1), :] = jnp.where(lane >= at, turned, 0.0)
    line[pl.ds(row + 1, 1), :] = jnp.where(lane < at, turned, line[pl.ds(row + 1, 1), :])
    for to in (keep, give):
        to[ROWS : ROWS + 8, 0:512] = line[...].astype(jnp.bfloat16)
    for copy in copies[:12]:
        copy.wait()

    rows = slice(0, ROWS)

    def fill(first, second):
        first[rows, 0:1024] = latest(tq, lq, hq)
        first[rows, 1024:1536] = latest(tk, lk, hk)
        second[rows, 0:512] = latest(tv, lv, hv)
        second[rows, 512:1536] = latest(tm, lm, hm)

    @pl.when(c == 0)
    def _():
        fill(keep, give)

    @pl.when(c == 1)
    def _():
        fill(give, keep)


def merge(*args):
    piece = pltpu.VMEM((ROWS + 8, HALF), jnp.bfloat16)
    return pl.pallas_call(
        merge_kernel,
        out_shape=(piece, piece),
        in_specs=anywhere(len(args)),
        out_specs=tuple(vmem(2)),
        scratch_shapes=[pltpu.VMEM(shape, a.dtype) for shape, a in zip(MERGED, args)]
        + [pltpu.VMEM(TILE, jnp.float32), pltpu.SemaphoreType.DMA((14,))],
        compiler_params=pltpu.CompilerParams(vmem_limit_bytes=8 * 2**20),
        name="merge",
    )(*[pltpu.with_memory_space_constraint(a, pltpu.HBM) for a in args])


def pair_kernel(keep, beside, out):
    _, _, c = place()
    for piece, core in ((keep, c), (beside, 1 - c)):
        out[pl.ds(pl.multiple_of(core * ROWS, 16), ROWS), :] = piece[0:ROWS, :]


def pair_of(keep, beside):
    return pl.pallas_call(
        pair_kernel,
        out_shape=pltpu.VMEM((STRIP, HALF), jnp.bfloat16),
        in_specs=vmem(2),
        out_specs=pl.BlockSpec(memory_space=pltpu.VMEM),
        compiler_params=pltpu.CompilerParams(vmem_limit_bytes=2 * 2**20),
        name="pair",
    )(*held((keep, beside)))


OFFSETS = ((3, 0), (1, 0), (3, 1), (1, 1), (2, 0), (2, 1))


def place_pieces(pieces, units, spots):
    _, _, c = place()
    for piece, (k, other) in zip(pieces, OFFSETS):
        core = c if other == 0 else 1 - c
        for j in range(3):
            if (j, k) in spots:
                unit, row, _ = spot(j, k)
                at = pl.multiple_of(row + core * ROWS, 16)
                units[unit][pl.ds(at, ROWS), :] = piece[0:ROWS, j * CHUNK : (j + 1) * CHUNK]


def near_kernel(*refs):
    place_pieces(refs[:4], {0: refs[4]}, ((0, 1), (0, 3)))


def known(*tiles):
    found = tiles[0].astype(jnp.float32)
    for tile in tiles[1:]:
        found = jnp.where(found != 0, found, tile.astype(jnp.float32))
    return found


def rest_kernel(*refs):
    pieces, one, two, tile = refs[:8], refs[8], refs[9], refs[10]
    spots = [(j, k) for j in (1, 2) for k in (1, 2, 3)] + [(0, 2)]
    place_pieces(pieces[:6], {1: one, 2: two}, spots)
    tile[...] = known(*[p[ROWS : ROWS + 8, 0:512] for p in pieces]).astype(tile.dtype)


def stack(kernel, pieces, shapes):
    return pl.pallas_call(
        kernel,
        out_shape=tuple(pltpu.VMEM(shape, jnp.bfloat16) for shape in shapes),
        in_specs=vmem(len(pieces)),
        out_specs=tuple(vmem(len(shapes))),
        compiler_params=pltpu.CompilerParams(vmem_limit_bytes=4 * 2**20),
    )(*held(pieces))


NAMES = ("query", "key", "mixed")
SHAPES = {"query": (1024, 3584), "key": (512, 3584), "mixed": (3584, 1024)}


def lay_kernel(work, sides, keys, n_in, *refs):
    n = len(keys)
    units = {side: dict(zip(keys, refs[i * n :])) for i, side in enumerate(sides)}
    own, partner, refs = units.get("own"), units.get("partner"), refs[len(sides) * n + n_in :]
    outs, (whole, turned, sems) = dict(zip(NAMES, refs[:3])), refs[3:]
    y, x, c = place()

    def lay(route0, route1):
        started = []

        def start(source, target):
            copy = pltpu.make_async_copy(source, target, sems.at[len(started)])
            copy.start()
            started.append(copy)

        for step, j in work if route1 else ():
            name, first = ROUTE1[j]
            if name == "mixed":
                g = (x + step + 4) % 4
                for k in range(4):
                    row = pl.multiple_of(((y + k) % 4) * GROUP + g * STRIP, 16)
                    unit, at, column = spot(j, k)
                    start(
                        route1[step, unit].at[pl.ds(at, STRIP), pl.ds(column, CHUNK)],
                        outs[name].at[pl.ds(row, STRIP), pl.ds(first, CHUNK)],
                    )
        for i, (step, j) in enumerate(work if route0 else ()):
            name, first = ROUTE0[j]
            for k in range(4):
                row = pl.multiple_of(((x + k) % 4) * STRIP, 16)
                unit, at, column = spot(j, k)
                whole[i, pl.ds(row, STRIP), :] = route0[step, unit][
                    at : at + STRIP, column : column + CHUNK
                ]
            column = pl.multiple_of(((y + step + 4) % 4) * GROUP, 128)
            for at in range(0, CHUNK, PART):
                turned[i, at : at + PART, :] = whole[i, :, at : at + PART].T
                start(
                    turned.at[i, pl.ds(at, PART), :],
                    outs[name].at[pl.ds(first + at, PART), pl.ds(column, GROUP)],
                )
        for copy in started:
            copy.wait()

    @pl.when(c == 0)
    def _():
        lay(own, partner)

    @pl.when(c == 1)
    def _():
        lay(partner, own)


BOTH = ("own", "partner")
LAID = (
    (((0, 0), (0, 1), (0, 2)), BOTH),
    (((-1, 0), (-1, 2), (1, 1)), BOTH),
    (((1, 0), (1, 2)), BOTH),
    (((2, 0), (2, 2)), BOTH),
    (((-1, 1), (2, 1)), ("own",)),
    (((-1, 1), (2, 1)), ("partner",)),
)


def lay(work, sides, mine, theirs, before):
    n = len(work)
    n_in = 0 if before is None else 3
    shapes = tuple(jax.ShapeDtypeStruct(SHAPES[name], jnp.bfloat16) for name in NAMES)
    keys = tuple(dict.fromkeys((s, u) for s, j in work for u in UNITS_OF[j]))
    by_side = {"own": mine, "partner": theirs}
    units = [by_side[side][s][u] for side in sides for s, u in keys]
    return pl.pallas_call(
        lambda *refs: lay_kernel(work, sides, keys, n_in, *refs),
        out_shape=shapes,
        in_specs=vmem(len(units)) + anywhere(n_in),
        out_specs=tuple(anywhere(3)),
        scratch_shapes=[
            pltpu.VMEM((n, GROUP, CHUNK), jnp.bfloat16),
            pltpu.VMEM((n, CHUNK, GROUP), jnp.bfloat16),
            pltpu.SemaphoreType.DMA((8 * n,)),
        ],
        input_output_aliases={len(units) + i: i for i in range(n_in)},
        compiler_params=pltpu.CompilerParams(vmem_limit_bytes=10 * 2**20),
    )(*held(units), *(before or ()))


STEPS = (0, -1, 1, 2)
VALUE_KEYS = tuple((s, u) for s in STEPS for u in UNITS_OF[0])


def value_kernel(*refs):
    n = len(VALUE_KEYS)
    own, partner, refs = dict(zip(VALUE_KEYS, refs)), dict(zip(VALUE_KEYS, refs[n:])), refs[2 * n :]
    out, whole, turned, sems = refs
    y, x, c = place()

    def gather(route1):
        for step in STEPS:
            g = (x + step + 4) % 4
            for k in range(4):
                row = pl.multiple_of(((y + k) % 4) * GROUP + g * STRIP, 16)
                unit, at, column = spot(0, k)
                whole[pl.ds(row, STRIP), :] = route1[step, unit][
                    at : at + STRIP, column : column + CHUNK
                ]

    @pl.when(c == 0)
    def _():
        gather(partner)

    @pl.when(c == 1)
    def _():
        gather(own)

    copies = []
    for s in range(4):
        turned[s] = whole[s * GROUP : (s + 1) * GROUP, :].T
        copy = pltpu.make_async_copy(turned.at[s], out.at[:, pl.ds(s * GROUP, GROUP)], sems.at[s])
        copy.start()
        copies.append(copy)
    for copy in copies:
        copy.wait()


def value_of(units):
    return pl.pallas_call(
        value_kernel,
        out_shape=jax.ShapeDtypeStruct((512, 3584), jnp.bfloat16),
        in_specs=vmem(2 * len(VALUE_KEYS)),
        out_specs=pl.BlockSpec(memory_space=pl.ANY),
        scratch_shapes=[
            pltpu.VMEM((3584, 512), jnp.bfloat16),
            pltpu.VMEM((4, 512, GROUP), jnp.bfloat16),
            pltpu.SemaphoreType.DMA((4,)),
        ],
        compiler_params=pltpu.CompilerParams(vmem_limit_bytes=10 * 2**20),
        name="value",
    )(*held(units))


def join_kernel(here, there, out):
    out[...] = known(here[...], there[...]).astype(jnp.bfloat16)


def norm_kernel(here, there, out, rows):
    found = known(here[...], there[...])
    for r in range(28):
        rows[r : r + 1, :] = found[r // 4 : r // 4 + 1, r % 4 * 128 : (r % 4 + 1) * 128]
    out[...] = rows[0:28, :].astype(jnp.bfloat16)


NEAR, ACROSS = (1, 0, 3, 2), (3, 2, 1, 0)


def along_first(partners):
    return pairs(lambda y, x, c: (y, partners[x], c) if c == 0 else (partners[y], x, c))


def norm_of(tile):
    moves = (
        ("width", list(enumerate(ACROSS))), ("width", list(enumerate(NEAR))),
        (ZERO, PARTNER), (ZERO, along_first(NEAR)), (ZERO, along_first(ACROSS)),
    )
    for k, (axis, move) in enumerate(moves):
        there = lax.ppermute(tile, axis, move)
        if k < 4:
            (tile,) = stack(join_kernel, (tile, there), (TILE,))
    return pl.pallas_call(
        norm_kernel,
        out_shape=jax.ShapeDtypeStruct((28, 128), jnp.bfloat16),
        in_specs=vmem(2),
        out_specs=pl.BlockSpec(memory_space=pltpu.VMEM),
        scratch_shapes=[pltpu.VMEM((32, 128), jnp.float32)],
        compiler_params=pltpu.CompilerParams(vmem_limit_bytes=2 * 2**20),
        name="norm",
    )(*held((tile, there))).reshape(-1)


def body(
    train_query,
    low_query,
    high_query,
    train_key,
    low_key,
    high_key,
    train_value,
    low_value,
    high_value,
    train_mixed,
    low_mixed,
    high_mixed,
    norm_train,
    norm_step,
):
    keep, give = merge(
        train_query,
        low_query.T,
        high_query,
        train_key,
        low_key.T,
        high_key,
        train_value,
        low_value.T,
        high_value,
        train_mixed.T,
        high_mixed,
        low_mixed.T,
        norm_train.reshape(1, NORM),
        norm_step.reshape(1, NORM),
    )
    beside = send(give, PARTNER)
    keep_up = send(keep, first_axis(1))
    give_down = send(give, first_axis_across(-1))
    keep_down = send(keep, first_axis(-1))
    give_up = send(give, first_axis_across(1))
    far_keep = send(keep_up, first_axis(1))
    far_give = send(give_down, first_axis(-1))
    pieces = (keep_up, keep_down, give_up, give_down, far_keep, far_give)
    (near,) = stack(near_kernel, pieces[:4], ((2 * STRIP, CHUNK),))
    shapes = ((REST, CHUNK), (REST + STRIP, CHUNK), TILE)
    *rest, tile = stack(rest_kernel, (*pieces, keep, beside), shapes)
    units = (near, *rest, pair_of(keep, beside))
    mine = {
        0: units,
        -1: [send(u, second_axis(1)) for u in units],
        1: [send(u, second_axis(-1)) for u in units],
    }
    mine[2] = [
        send(mine[-1][j], second_axis(1))
        if j in (0, 2)
        else send(mine[1][j], second_axis(-1))
        for j in range(4)
    ]
    theirs = {s: [send(u, PARTNER) for u in mine[s]] for s in STEPS}

    outs = None
    for work, sides in LAID:
        outs = lay(work, sides, mine, theirs, outs)
    ready_query, ready_key, ready_mixed = outs
    ready_value = value_of([side[s][u] for side in (mine, theirs) for s, u in VALUE_KEYS])

    serve_norm = norm_of(tile)
    return (ready_query, ready_key, ready_value, ready_mixed, serve_norm)


def solution(mesh):
    torus = Mesh(
        mesh.devices.reshape(4, 4, 2, mesh.shape["width"]), ("zero_0", "zero_1", "zero_2", "width")
    )
    return jax.shard_map(
        body,
        mesh=torus,
        in_specs=(
            P(ZERO, "width"),
            P(ZERO, None),
            P(None, "width"),
            P(ZERO, "width"),
            P(ZERO, None),
            P(None, "width"),
            P(ZERO, "width"),
            P(ZERO, None),
            P(None, "width"),
            P("width", ZERO),
            P("width", None),
            P(None, ZERO),
            P(ZERO_WIDTH),
            P(ZERO_WIDTH),
        ),
        out_specs=(P("width", None), P("width", None), P("width", None), P(None, "width"), P()),
        check_vma=False,
    )
```
